32 devices in a mesh: strip: 8 (over z, x), col: 4 (over y, core).
Axes of the slice: x: 2, y: 2, z: 4, core: 2. Of those that a mesh axis runs over, the one named last changes fastest.
Arguments:
- residuals: float32 [16, 64, 2560], P('strip'), may hold values from -6 to 6
- corr_rows: float32 [64], replicated, may hold values from 0.5 to 2
- corr_cols: float32 [2560], replicated, may hold values from 0.5 to 2
- row_anchor: int32 [16], replicated, may hold values from 0 to 64
- col_anchor: int32 [16], replicated, may hold values from 0 to 7680
- valid_first: int32 [16], replicated, may hold values from 0 to 15
- valid_end: int32 [16], replicated, may hold values from 49 to 64
- facet_of_slot: int32 [16], replicated, may hold values from 0 to 15, each once
Outputs:
- stitched: float32 [128, 10240], P('strip', 'col')
- column_power: float32 [10240], P('col')
The draws below stay inside these ranges and needn't reach their ends.
Inputs may be any that keep to these rules, and one draw needn't show every extreme that they name: facet_of_slot names each of the 16 facets exactly once.
All inputs are finite; a program needn't handle non-finite values.
Results may differ from the reference program's by a relative error of at most 0.0003.
Values sent between devices are 32-bit elements; how exact they have to be, the bound alone decides.
A program may use at most 64 MiB of HBM per device.

```python
import math
import jax
import jax.numpy as jnp
from jax import lax

FW = 2560
FH = 64
FACETS = 16
MH = 128
MW = 10240


def with_ends(array, stream_key, low, largest):
    place = [jax.random.randint(jax.random.fold_in(stream_key, axis), (), 0, length) for axis, length in enumerate(array.shape)]
    longest = array.shape.index(max(array.shape))
    neighbour = place[:longest] + [(place[longest] + 1) % array.shape[longest]] + place[longest + 1:]
    return array.at[tuple(place)].set(low).at[tuple(neighbour)].set(largest)


def level_of(rng, shape, shards, smallest, high):
    loudness, own = 1.0, jax.random.fold_in(rng, 6)
    for dim, parts in shards:
        steps = jnp.exp(jax.random.uniform(jax.random.fold_in(own, dim), (parts,), jnp.float32, smallest / len(shards), high / len(shards)))
        loudness = loudness * jnp.repeat(steps, shape[dim] // parts).reshape([-1 if axis == dim else 1 for axis in range(len(shape))])
    return loudness


def scatter_about(rng, extent, deviation, most, split=(), dtype=jnp.bfloat16):
    entries = jax.random.normal(rng, extent, jnp.float32) * deviation
    if len(split) > 0:
        entries = level_of(rng, extent, split, -0.22, 0.18) * entries
    return jnp.clip(entries, min=-most, max=most).astype(dtype)


def setup_inputs(seed: int = 0) -> dict:
    keys = jax.random.split(jax.random.key(seed), 9)
    residuals = scatter_about(keys[0], (FACETS, FH, FW), 1.0, 6.0, ((0, 8),), jnp.float32)
    corr_rows = jnp.clip(jnp.exp(jax.random.uniform(keys[1], (FH,), jnp.float32, math.log(0.5), math.log(2.0))), 0.5, 2.0)
    corr_cols = jnp.clip(jnp.exp(jax.random.uniform(keys[2], (FW,), jnp.float32, math.log(0.5), math.log(2.0))), 0.5, 2.0)
    row_anchor = with_ends(jax.random.randint(keys[3], (FACETS,), 0, MH - FH + 1), jax.random.fold_in(keys[3], 1), 0, MH - FH).astype(jnp.int32)
    col_anchor = with_ends(jax.random.randint(keys[4], (FACETS,), 0, MW - FW + 1), jax.random.fold_in(keys[4], 1), 0, MW - FW).astype(jnp.int32)
    valid_first = with_ends(jax.random.randint(keys[5], (FACETS,), 0, FH // 4), jax.random.fold_in(keys[5], 1), 0, (FH // 4) - 1).astype(jnp.int32)
    valid_end = with_ends(jax.random.randint(keys[6], (FACETS,), 3 * FH // 4 + 1, FH + 1), jax.random.fold_in(keys[6], 1), 3 * FH // 4 + 1, FH).astype(jnp.int32)
    facet_of_slot = jax.random.permutation(keys[7], FACETS).astype(jnp.int32)
    return dict(residuals=residuals, corr_rows=corr_rows, corr_cols=corr_cols, row_anchor=row_anchor, col_anchor=col_anchor, valid_first=valid_first, valid_end=valid_end, facet_of_slot=facet_of_slot)


def tapers(count):
    position = (jnp.arange(count).astype(jnp.float32) + 0.5) / count
    return jnp.sin(jnp.pi * position) ** 2


def reference(residuals, corr_rows, corr_cols, row_anchor, col_anchor, valid_first, valid_end, facet_of_slot):
    facet_rows = residuals.shape[1]
    facet_cols = residuals.shape[2]
    row_index = jnp.arange(facet_rows).astype(jnp.int32)
    row_taper = tapers(facet_rows)
    col_taper = tapers(facet_cols)
    correction = corr_rows[:, None] * corr_cols[None, :]

    def accumulate(running, position):
        numerator, denominator = running
        facet_id = facet_of_slot[position]
        row_start = row_anchor[facet_id]
        col_start = col_anchor[facet_id]
        inside = (row_index >= valid_first[facet_id]) & (row_index < valid_end[facet_id])
        row_weight = jnp.where(inside, row_taper, 0.0)
        weight = row_weight[:, None] * col_taper[None, :]
        weighted = weight * correction * residuals[position]
        old_num = lax.dynamic_slice(numerator, (row_start, col_start), (facet_rows, facet_cols))
        numerator = lax.dynamic_update_slice(numerator, old_num + weighted, (row_start, col_start))
        old_den = lax.dynamic_slice(denominator, (row_start, col_start), (facet_rows, facet_cols))
        denominator = lax.dynamic_update_slice(denominator, old_den + weight, (row_start, col_start))
        return (numerator, denominator), None

    blank = jnp.zeros((MH, MW), jnp.float32)
    (numerator, denominator), _ = lax.scan(accumulate, (blank, blank), jnp.arange(FACETS).astype(jnp.int32))
    stitched = numerator / jnp.maximum(denominator, 0.5)
    column_power = jnp.mean(stitched * stitched, axis=0)
    return (stitched, column_power)
```

```python
import functools
import math

import jax
import jax.numpy as jnp
from jax import lax
from jax.experimental import pallas as pl
from jax.experimental.pallas import tpu as pltpu
from jax.sharding import PartitionSpec as P

MESH = pl.DeviceIdType.MESH
CHUNKS = 4
EARLY = 0.15
TILE = 128


def taper(position, count):
    angle = (position.astype(jnp.float32) + (0.5 - count / 2)) * (math.pi / count)
    square = angle * angle
    value = jnp.full_like(square, 1.0 / math.factorial(12))
    for order in (10, 8, 6, 4, 2, 0):
        sign = -1.0 if order % 4 == 2 else 1.0
        value = value * square + sign / math.factorial(order)
    return value * value


def visit_order(count):
    return [sorted(range(count), key=lambda d: (-abs(d - z), d < z)) for z in range(count)]


def column_chunks(tiles, first):
    edges = [first + (tiles - first) * c // CHUNKS for c in range(CHUNKS + 1)]
    return [(a, b - a) for a, b in zip(edges, edges[1:]) if b > a]


def kernel(
    strips, lanes,
    slots_ref, row_ref, col_ref, first_ref, end_ref, rows_hbm, cols_hbm, res_hbm,
    out_ref, power_ref,
    res_ref, rows_ref, cols_ref, rolled, blocks, inv, xrecv, zsend, zrecv,
    fsend, frecv, fkeep, fxsend, fxrecv, psend, precv,
    in_sem, xs_sem, xr_sem, zs_sem, zr_sem, fs_sem, fr_sem, gs_sem, gr_sem, ps_sem, pr_sem,
):
    local, fh, fw = res_ref.shape
    facets = slots_ref.shape[0]
    height = out_ref.shape[0]
    levels = strips // lanes
    tiles = fw // TILE
    early = fsend.shape[2]
    chunks = column_chunks(tiles, early)
    parts = [(0, early)] + chunks
    strip = lax.axis_index("strip")
    group = lax.axis_index("col")
    z, x = lax.div(strip, lanes), lax.rem(strip, lanes)

    loads = [
        pltpu.make_async_copy(rows_hbm, rows_ref, in_sem.at[0]),
        pltpu.make_async_copy(cols_hbm, cols_ref, in_sem.at[1]),
    ] + [
        pltpu.make_async_copy(res_hbm.at[p], res_ref.at[p], in_sem.at[2 + p])
        for p in range(local)
    ]
    for load in loads:
        load.start()

    barrier = pltpu.get_barrier_semaphore()
    for k in range(1, strips):
        peer = lax.rem(strip + k, strips)
        pl.semaphore_signal(barrier, inc=1, device_id={"strip": peer}, device_id_type=MESH)

    order = visit_order(levels)

    def dest(t):
        d = jnp.int32(order[0][t])
        for place_z in range(1, levels):
            d = jnp.where(z == place_z, jnp.int32(order[place_z][t]), d)
        return d

    def lane_of(k):
        return lax.rem(x + k, lanes)

    def span(c):
        return pl.ds(chunks[c][0], chunks[c][1])

    def x_copy(k, d, c):
        return pltpu.make_async_remote_copy(
            src_ref=blocks.at[d, lane_of(k), span(c)],
            dst_ref=xrecv.at[k - 1, d, span(c)],
            send_sem=xs_sem.at[k - 1, d, c],
            recv_sem=xr_sem.at[k - 1, d, c],
            device_id={"strip": z * lanes + lane_of(k)},
            device_id_type=MESH,
        )

    def z_copy(way, d, c, target):
        return pltpu.make_async_remote_copy(
            src_ref=zsend.at[d, span(c)],
            dst_ref=zrecv.at[way, d, span(c)],
            send_sem=zs_sem.at[d, c],
            recv_sem=zr_sem.at[way, d, c],
            device_id={"strip": target * lanes + x},
            device_id_type=MESH,
        )

    def f_copy(way, d, target):
        return pltpu.make_async_remote_copy(
            src_ref=fsend.at[d],
            dst_ref=frecv.at[way, d],
            send_sem=fs_sem.at[d],
            recv_sem=fr_sem.at[way, d],
            device_id={"strip": target * lanes + x},
            device_id_type=MESH,
        )

    def g_copy(k):
        return pltpu.make_async_remote_copy(
            src_ref=fxsend.at[k - 1],
            dst_ref=fxrecv.at[k - 1],
            send_sem=gs_sem.at[k - 1],
            recv_sem=gr_sem.at[k - 1],
            device_id={"strip": z * lanes + lane_of(k)},
            device_id_type=MESH,
        )

    def p_copy(k, i):
        return pltpu.make_async_remote_copy(
            src_ref=psend.at[pl.ds(*parts[i])],
            dst_ref=precv.at[k - 1, pl.ds(*parts[i])],
            send_sem=ps_sem.at[k - 1, i],
            recv_sem=pr_sem.at[k - 1, i],
            device_id={"strip": lax.rem(strip + k, strips)},
            device_id_type=MESH,
        )

    eye = lax.broadcasted_iota(jnp.int32, (fh, fh), 0) == lax.broadcasted_iota(
        jnp.int32, (fh, fh), 1
    )
    y = lax.broadcasted_iota(jnp.int32, (fh, 1), 0)
    u = lax.broadcasted_iota(jnp.int32, (1, fw), 1)
    row_taper = taper(y, fh)
    col_taper = taper(u, fw)
    loads[0].wait()
    loads[1].wait()
    corr_row = jnp.sum(jnp.where(eye, rows_ref[...], 0.0), axis=1, keepdims=True)
    corr_col = jnp.concatenate([cols_ref[pl.ds(i, 1), :] for i in range(tiles)], axis=1)
    col_scale = col_taper * corr_col
    anchors = []
    for p in range(local):
        f = slots_ref[strip * local + p]
        ra, ca = row_ref[f], col_ref[f]
        anchors.append(ra)
        inside = (y >= first_ref[f]) & (y < end_ref[f])
        row_scale = jnp.where(inside, row_taper, 0.0) * corr_row
        col_pos = u + (group * fw - ca)
        col_inside = (col_pos >= 0) & (col_pos < fw)
        shift = lax.rem(ca, fw)
        loads[2 + p].wait()
        for row in range(0, fh, 8):
            term = res_ref[p, pl.ds(row, 8), :] * col_scale * row_scale[row : row + 8]
            rolled[p, pl.ds(row, 8), :] = jnp.where(col_inside, pltpu.roll(term, shift, axis=1), 0.0)
    spare = jnp.zeros((strips * height - fh, TILE), jnp.float32)
    for j in range(tiles):
        total = None
        for p in range(local):
            piece = jnp.concatenate([rolled[p, :, pl.ds(j * TILE, TILE)], spare], axis=0)
            piece = pltpu.roll(piece, anchors[p], axis=0)
            total = piece if total is None else total + piece
        for s in range(strips):
            blocks[s // lanes, s % lanes, j] = total[s * height : (s + 1) * height]

    pl.semaphore_wait(barrier, strips - 1)
    for t in range(levels - 1):
        d = dest(t)
        right = d > z
        fed = jnp.where(right, z > 0, z < levels - 1)
        fsend[d] = blocks[d, :, pl.ds(0, early)]

        @pl.when(jnp.logical_not(fed))
        def _():
            f_copy(jnp.where(right, 0, 1), d, jnp.where(right, z + 1, z - 1)).start()

    for t in range(levels):
        d = dest(t)
        for c in range(len(chunks)):
            for k in range(1, lanes):
                x_copy(k, d, c).start()

    v = lax.broadcasted_iota(jnp.int32, (height, 1), 0) + strip * height
    u8 = lax.broadcasted_iota(jnp.int32, (8, fw), 1) + group * fw
    inv[...] = jnp.zeros_like(inv)

    def add_facet(f, carry):
        row_pos = v - row_ref[f]
        row_inside = (row_pos >= first_ref[f]) & (row_pos < end_ref[f])
        row_part = jnp.where(row_inside, taper(row_pos, fh), 0.0)
        col_pos = u8 - col_ref[f]
        col_inside = (col_pos >= 0) & (col_pos < fw)
        col_part = jnp.where(col_inside, taper(col_pos, fw), 0.0)
        for j in range(tiles):
            for row in range(0, height, 8):
                inv[j, pl.ds(row, 8), :] += (
                    row_part[row : row + 8] * col_part[:, j * TILE : (j + 1) * TILE]
                )
        return carry

    lax.fori_loop(0, facets, add_facet, 0)
    inv[...] = 1.0 / jnp.maximum(inv[...], 0.5)

    def gather_x(d, c):
        total = blocks[d, x, span(c)]
        for k in range(1, lanes):
            x_copy(k, d, c).wait_recv()
            total = total + xrecv[k - 1, d, span(c)]
        return total

    def pass_early(t):
        d = dest(t)
        right = d > z
        way = jnp.where(right, 0, 1)
        target = jnp.where(right, z + 1, z - 1)
        fed = jnp.where(right, z > 0, z < levels - 1)

        @pl.when(fed)
        def _():
            f_copy(way, d, target).wait_recv()
            fsend[d] += frecv[way, d]
            f_copy(way, d, target).start()

    def pass_rest(t):
        d = dest(t)
        right = d > z
        way = jnp.where(right, 0, 1)
        target = jnp.where(right, z + 1, z - 1)
        fed = jnp.where(right, z > 0, z < levels - 1)
        for c in range(len(chunks)):
            zsend[d, span(c)] = gather_x(d, c)

            @pl.when(fed)
            def _():
                z_copy(way, d, c, target).wait_recv()
                zsend[d, span(c)] += zrecv[way, d, span(c)]

            z_copy(way, d, c, target).start()

    def swap_early():
        fkeep[...] = blocks[z, :, pl.ds(0, early)]

        @pl.when(z > 0)
        def _():
            f_copy(0, z, z - 1).wait_recv()
            fkeep[...] += frecv[0, z]

        @pl.when(z < levels - 1)
        def _():
            f_copy(1, z, z + 1).wait_recv()
            fkeep[...] += frecv[1, z]

        for k in range(1, lanes):
            fxsend[k - 1] = fkeep[lane_of(k)]
        for k in range(1, lanes):
            g_copy(k).start()

    def settle(i, total):
        first, count = parts[i]
        stitched = total * inv[pl.ds(first, count)]
        for j in range(count):
            out_ref[:, pl.ds((first + j) * TILE, TILE)] = stitched[j]
        psend[pl.ds(first, count)] = jnp.sum(stitched * stitched, axis=1, keepdims=True)
        for k in range(1, strips):
            p_copy(k, i).start()

    for t in range(levels - 1):
        if t == 0:
            pass_early(0)
        if t == min(1, levels - 2):
            for later in range(1, levels - 1):
                pass_early(later)
        if t == levels - 2:
            swap_early()
        pass_rest(t)

    for c in range(len(chunks)):
        zsend[z, span(c)] = gather_x(z, c)

        @pl.when(z > 0)
        def _():
            z_copy(0, z, c, z - 1).wait_recv()
            zsend[z, span(c)] += zrecv[0, z, span(c)]

        @pl.when(z < levels - 1)
        def _():
            z_copy(1, z, c, z + 1).wait_recv()
            zsend[z, span(c)] += zrecv[1, z, span(c)]

        settle(1 + c, zsend[z, span(c)])
    total = fkeep[x]
    for k in range(1, lanes):
        g_copy(k).wait_recv()
        total = total + fxrecv[k - 1]
    settle(0, total)

    for i in range(len(parts)):
        for k in range(1, strips):
            p_copy(k, i).wait_recv()
    total = psend[...]
    for k in range(1, strips):
        total = total + precv[k - 1]
    total = total * (1.0 / (strips * height))
    for j in range(tiles):
        power_ref[pl.ds(j, 1), :] = total[j]

    for i in range(len(parts)):
        for k in range(1, strips):
            p_copy(k, i).wait_send()
    for k in range(1, lanes):
        g_copy(k).wait_send()
    for t in range(levels):
        d = dest(t)
        target = jnp.where(d > z, z + 1, z - 1)
        for c in range(len(chunks)):
            for k in range(1, lanes):
                x_copy(k, d, c).wait_send()
            if t < levels - 1:
                z_copy(0, d, c, target).wait_send()
        if t < levels - 1:
            f_copy(0, d, target).wait_send()


def finish(stitched_ref, power_ref, out_ref, power_out, sems):
    copies = [
        pltpu.make_async_copy(stitched_ref, out_ref, sems.at[0]),
        pltpu.make_async_copy(power_ref, power_out, sems.at[1]),
    ]
    for copy in copies:
        copy.start()
    for copy in copies:
        copy.wait()


def body(strips, lanes, residuals, corr_rows, corr_cols, row_anchor, col_anchor, first, end, slots):
    local, fh, fw = residuals.shape
    height = fh // 4
    levels = strips // lanes
    others = max(lanes - 1, 1)
    smem = pl.BlockSpec(memory_space=pltpu.SMEM)
    vmem = pl.BlockSpec(memory_space=pltpu.VMEM)
    hbm = pl.BlockSpec(memory_space=pltpu.HBM)
    dma = pltpu.SemaphoreType.DMA
    tiles = fw // TILE
    early = max(round(EARLY * tiles), 1)
    chunks = len(column_chunks(tiles, early))
    block_bytes = 4 * height * fw
    margin = 4 * 1024 * 1024
    blocks = 8 * local + (2 + others) * strips + 4 * levels + 4
    stitched, power = pl.pallas_call(
        functools.partial(kernel, strips, lanes),
        out_shape=(
            jax.ShapeDtypeStruct((height, fw), jnp.float32),
            jax.ShapeDtypeStruct((tiles, TILE), jnp.float32),
        ),
        in_specs=[smem] * 5 + [hbm] * 3,
        out_specs=(vmem, vmem),
        scratch_shapes=[
            pltpu.VMEM((local, fh, fw), jnp.float32),
            pltpu.VMEM((1, fh), jnp.float32),
            pltpu.VMEM((tiles, TILE), jnp.float32),
            pltpu.VMEM((local, fh, fw), jnp.float32),
            pltpu.VMEM((levels, lanes, tiles, height, TILE), jnp.float32),
            pltpu.VMEM((tiles, height, TILE), jnp.float32),
            pltpu.VMEM((others, levels, tiles, height, TILE), jnp.float32),
            pltpu.VMEM((levels, tiles, height, TILE), jnp.float32),
            pltpu.VMEM((2, levels, tiles, height, TILE), jnp.float32),
            pltpu.VMEM((levels, lanes, early, height, TILE), jnp.float32),
            pltpu.VMEM((2, levels, lanes, early, height, TILE), jnp.float32),
            pltpu.VMEM((lanes, early, height, TILE), jnp.float32),
            pltpu.VMEM((others, early, height, TILE), jnp.float32),
            pltpu.VMEM((others, early, height, TILE), jnp.float32),
            pltpu.VMEM((tiles, 1, TILE), jnp.float32),
            pltpu.VMEM((strips - 1, tiles, 1, TILE), jnp.float32),
            dma((2 + local,)),
            dma((others, levels, chunks)),
            dma((others, levels, chunks)),
            dma((levels, chunks)),
            dma((2, levels, chunks)),
            dma((levels,)),
            dma((2, levels)),
            dma((others,)),
            dma((others,)),
            dma((strips - 1, chunks + 1)),
            dma((strips - 1, chunks + 1)),
        ],
        compiler_params=pltpu.CompilerParams(
            collective_id=0,
            has_side_effects=True,
            vmem_limit_bytes=blocks * block_bytes + margin,
        ),
    )(*(
        pltpu.with_memory_space_constraint(operand, pltpu.HBM)
        for operand in (
            slots, row_anchor, col_anchor, first, end,
            corr_rows[None, :], corr_cols.reshape(fw // TILE, TILE), residuals,
        )
    ))
    stitched, power = pl.pallas_call(
        finish,
        out_shape=(
            jax.ShapeDtypeStruct((height, fw), jnp.float32),
            jax.ShapeDtypeStruct((fw // TILE, TILE), jnp.float32),
        ),
        in_specs=[vmem, vmem],
        out_specs=(hbm, hbm),
        scratch_shapes=[dma((2,))],
    )(*(pltpu.with_memory_space_constraint(part, pltpu.VMEM) for part in (stitched, power)))
    return stitched, power.reshape(fw)


def solution(mesh):
    strips = mesh.shape["strip"]
    lanes = math.gcd(strips, max(mesh.shape["col"] // 2, 1))
    in_specs = (P("strip", None, None), P(), P(), P(), P(), P(), P(), P())
    out_specs = (P("strip", "col"), P("col"))
    run = functools.partial(body, strips, lanes)
    return jax.shard_map(run, mesh=mesh, in_specs=in_specs, out_specs=out_specs, check_vma=False)
```

```python
import functools
import math

import jax
import jax.numpy as jnp
from jax import lax
from jax.experimental import pallas as pl
from jax.experimental.pallas import tpu as pltpu
from jax.sharding import PartitionSpec as P

MESH = pl.DeviceIdType.MESH
CHUNKS = 4
EARLY = 0.15
TILE = 128


def taper(position, count):
    angle = (position.astype(jnp.float32) + (0.5 - count / 2)) * (math.pi / count)
    square = angle * angle
    value = jnp.full_like(square, 1.0 / math.factorial(12))
    for order in (10, 8, 6, 4, 2, 0):
        sign = -1.0 if order % 4 == 2 else 1.0
        value = value * square + sign / math.factorial(order)
    return value * value


def fed(levels, z, d):
    return (z == 1 < d) or (z == levels - 2 > d)


def visit_order(levels):
    return [
        sorted((d for d in range(levels) if d != z), key=lambda d: (fed(levels, z, d), -abs(d - z)))
        for z in range(levels)
    ]


def column_chunks(tiles, first):
    edges = [first + (tiles - first) * c // CHUNKS for c in range(CHUNKS + 1)]
    return [(a, b - a) for a, b in zip(edges, edges[1:]) if b > a]


def kernel(
    strips, lanes,
    slots_hbm, row_hbm, col_hbm, first_hbm, end_hbm, rows_hbm, cols_hbm, res_hbm,
    out_ref, power_ref,
    slots_ref, row_ref, col_ref, first_ref, end_ref, res_ref, rows_ref, cols_ref, rolled, blocks, inv, xrecv, zsend, zrecv,
    fsend, frecv, fkeep, fxsend, fxrecv, psend, precv,
    line, in_sem, xs_sem, xr_sem, zs_sem, zr_sem, fs_sem, fr_sem, gs_sem, gr_sem, ps_sem, pr_sem,
):
    local, fh, fw = res_ref.shape
    facets = slots_ref.shape[0]
    height = out_ref.shape[0]
    levels = strips // lanes
    tiles = fw // TILE
    early = fsend.shape[2]
    chunks = column_chunks(tiles, early)
    parts = [(0, early)] + chunks
    strip = lax.axis_index("strip")
    group = lax.axis_index("col")
    z, x = lax.div(strip, lanes), lax.rem(strip, lanes)

    sources = [
        (slots_hbm, slots_ref), (row_hbm, row_ref), (col_hbm, col_ref), (first_hbm, first_ref),
        (end_hbm, end_ref), (rows_hbm, rows_ref), (cols_hbm, cols_ref),
    ]
    small = len(sources)
    sources += [(res_hbm.at[p], res_ref.at[p]) for p in range(local)]
    loads = [
        pltpu.make_async_copy(source, target, in_sem.at[i])
        for i, (source, target) in enumerate(sources)
    ]
    for load in loads:
        load.start()

    low, high = z > 0, z < levels - 1
    leaf = jnp.logical_not(low & high)

    def at(level, lane):
        return {"strip": level * lanes + lane}

    barrier = pltpu.get_barrier_semaphore()
    for k in range(1, lanes):
        pl.semaphore_signal(barrier, device_id=at(z, lax.rem(x + k, lanes)), device_id_type=MESH)
    for there, step in ((low, -1), (high, 1)):

        @pl.when(there)
        def _():
            pl.semaphore_signal(barrier, device_id=at(z + step, x), device_id_type=MESH)

    def enter():
        pl.semaphore_wait(barrier, lanes - 1 + low.astype(jnp.int32) + high.astype(jnp.int32))
        for side, there, step in ((0, jnp.logical_not(low) & high, 1), (1, jnp.logical_not(high) & low, -1)):

            @pl.when(there)
            def _():
                pl.semaphore_signal(line.at[side], device_id=at(z + step, x), device_id_type=MESH)

    def hear(side, when):
        @pl.when(when)
        def _():
            pl.semaphore_wait(line.at[side], 1)

            @pl.when(high if side == 0 else low)
            def _():
                pl.semaphore_signal(
                    line.at[side], device_id=at(z + (1 if side == 0 else -1), x), device_id_type=MESH
                )

    order = visit_order(levels)

    def pick(values):
        value = jnp.int32(values[0])
        for level in range(1, levels):
            value = jnp.where(z == level, jnp.int32(values[level]), value)
        return value

    def dest(t):
        return pick([row[t] for row in order])

    def is_fed(t):
        return pick([int(fed(levels, level, row[t])) for level, row in enumerate(order)]) == 1

    def route(d):
        target = jnp.where(z == 0, min(1, levels - 1), jnp.where(high, d, levels - 2))
        slot = jnp.where(target == d, z, jnp.where(z == 0, levels + d, 2 * levels + d))
        return target, slot

    def inlet(d):
        return jnp.where(d > z, levels + d, 2 * levels + d)

    def sources():
        for level in range(levels):
            if 0 < level < levels - 1:
                yield level, z != level
            elif levels > 1:
                yield level, z == (1 if level == 0 else levels - 2)

    def lane_of(k):
        return lax.rem(x + k, lanes)

    def span(c):
        return pl.ds(chunks[c][0], chunks[c][1])

    def x_copy(k, d, c):
        return pltpu.make_async_remote_copy(
            src_ref=blocks.at[d, lane_of(k), span(c)],
            dst_ref=xrecv.at[k - 1, d, span(c)],
            send_sem=xs_sem.at[k - 1, d, c],
            recv_sem=xr_sem.at[k - 1, d, c],
            device_id=at(z, lane_of(k)),
            device_id_type=MESH,
        )

    def z_copy(d, c, target, slot):
        return pltpu.make_async_remote_copy(
            src_ref=zsend.at[d, span(c)],
            dst_ref=zrecv.at[slot, span(c)],
            send_sem=zs_sem.at[d, c],
            recv_sem=zr_sem.at[slot, c],
            device_id=at(target, x),
            device_id_type=MESH,
        )

    def f_copy(d, target, slot, source=None):
        return pltpu.make_async_remote_copy(
            src_ref=fsend.at[d] if source is None else source,
            dst_ref=frecv.at[slot],
            send_sem=fs_sem.at[d],
            recv_sem=fr_sem.at[slot],
            device_id=at(target, x),
            device_id_type=MESH,
        )

    def g_copy(k):
        return pltpu.make_async_remote_copy(
            src_ref=fxsend.at[k - 1],
            dst_ref=fxrecv.at[k - 1],
            send_sem=gs_sem.at[k - 1],
            recv_sem=gr_sem.at[k - 1],
            device_id=at(z, lane_of(k)),
            device_id_type=MESH,
        )

    def p_copy(k, i):
        return pltpu.make_async_remote_copy(
            src_ref=psend.at[pl.ds(*parts[i])],
            dst_ref=precv.at[k - 1, pl.ds(*parts[i])],
            send_sem=ps_sem.at[k - 1, i],
            recv_sem=pr_sem.at[k - 1, i],
            device_id={"strip": lax.rem(strip + k, strips)},
            device_id_type=MESH,
        )

    eye = lax.broadcasted_iota(jnp.int32, (fh, fh), 0) == lax.broadcasted_iota(
        jnp.int32, (fh, fh), 1
    )
    y = lax.broadcasted_iota(jnp.int32, (fh, 1), 0)
    u = lax.broadcasted_iota(jnp.int32, (1, fw), 1)
    row_taper = taper(y, fh)
    col_taper = taper(u, fw)
    for load in loads[:small]:
        load.wait()
    corr_row = jnp.sum(jnp.where(eye, rows_ref[...], 0.0), axis=1, keepdims=True)
    corr_col = jnp.concatenate([cols_ref[pl.ds(i, 1), :] for i in range(tiles)], axis=1)
    col_scale = col_taper * corr_col
    anchors = []
    for p in range(local):
        f = slots_ref[strip * local + p]
        ra, ca = row_ref[f], col_ref[f]
        anchors.append(ra)
        inside = (y >= first_ref[f]) & (y < end_ref[f])
        row_scale = jnp.where(inside, row_taper, 0.0) * corr_row
        col_pos = u + (group * fw - ca)
        col_inside = (col_pos >= 0) & (col_pos < fw)
        shift = lax.rem(ca, fw)
        loads[small + p].wait()
        for row in range(0, fh, 8):
            term = res_ref[p, pl.ds(row, 8), :] * col_scale * row_scale[row : row + 8]
            rolled[p, pl.ds(row, 8), :] = jnp.where(col_inside, pltpu.roll(term, shift, axis=1), 0.0)
    spare = jnp.zeros((strips * height - fh, TILE), jnp.float32)

    def place(j):
        total = None
        for p in range(local):
            piece = jnp.concatenate([rolled[p, :, pl.ds(j * TILE, TILE)], spare], axis=0)
            piece = pltpu.roll(piece, anchors[p], axis=0)
            total = piece if total is None else total + piece
        for s in range(strips):
            blocks[s // lanes, s % lanes, j] = total[s * height : (s + 1) * height]

    def open_early():
        for t in range(levels - 1):
            d = dest(t)
            target, slot = route(d)

            @pl.when(jnp.logical_not(is_fed(t)))
            def _():
                f_copy(d, target, slot, blocks.at[d, :, pl.ds(0, early)]).start()

    for i, (first, count) in enumerate(parts):
        for j in range(first, first + count):
            place(j)
            if j == first and i == 1:
                enter()
                open_early()
            if j == first and i > 1:
                for k in range(1, lanes):
                    x_copy(k, dest(0), i - 2).start()
    for k in range(1, lanes):
        x_copy(k, dest(0), len(chunks) - 1).start()
    for t in range(1, levels):
        for c in range(len(chunks)):
            for k in range(1, lanes):
                x_copy(k, dest(t) if t < levels - 1 else z, c).start()
    hear(0, (z == 1) & high)
    hear(1, (z == levels - 2) & low)

    v = lax.broadcasted_iota(jnp.int32, (height, 1), 0) + strip * height
    u8 = lax.broadcasted_iota(jnp.int32, (8, fw), 1) + group * fw
    inv[...] = jnp.zeros_like(inv)

    def add_facet(f, carry):
        row_pos = v - row_ref[f]
        row_inside = (row_pos >= first_ref[f]) & (row_pos < end_ref[f])
        row_part = jnp.where(row_inside, taper(row_pos, fh), 0.0)
        col_pos = u8 - col_ref[f]
        col_inside = (col_pos >= 0) & (col_pos < fw)
        col_part = jnp.where(col_inside, taper(col_pos, fw), 0.0)
        for j in range(tiles):
            for row in range(0, height, 8):
                inv[j, pl.ds(row, 8), :] += (
                    row_part[row : row + 8] * col_part[:, j * TILE : (j + 1) * TILE]
                )
        return carry

    lax.fori_loop(0, facets, add_facet, 0)
    inv[...] = 1.0 / jnp.maximum(inv[...], 0.5)
    hear(0, (z > 1) & high)
    hear(1, (z < levels - 2) & low)

    def gather_x(d, c):
        total = blocks[d, x, span(c)]
        for k in range(1, lanes):
            x_copy(k, d, c).wait_recv()
            total = total + xrecv[k - 1, d, span(c)]
        return total

    def pass_early(t):
        d = dest(t)
        target, slot = route(d)

        @pl.when(is_fed(t))
        def _():
            f_copy(d, z, inlet(d)).wait_recv()
            fsend[d] = blocks[d, :, pl.ds(0, early)] + frecv[inlet(d)]
            f_copy(d, target, slot).start()

    def pass_rest(t):
        d = dest(t)
        target, slot = route(d)
        for c in range(len(chunks)):
            zsend[d, span(c)] = gather_x(d, c)

            @pl.when(is_fed(t))
            def _():
                z_copy(d, c, z, inlet(d)).wait_recv()
                zsend[d, span(c)] += zrecv[inlet(d), span(c)]

            z_copy(d, c, target, slot).start()

    def swap_early():
        fkeep[...] = blocks[z, :, pl.ds(0, early)]
        for level, there in sources():

            @pl.when(there)
            def _():
                f_copy(z, z, level).wait_recv()
                fkeep[...] += frecv[level]

        for k in range(1, lanes):
            fxsend[k - 1] = fkeep[lane_of(k)]
        for k in range(1, lanes):
            g_copy(k).start()

    def settle(i, total):
        first, count = parts[i]
        stitched = total * inv[pl.ds(first, count)]
        for j in range(count):
            out_ref[:, pl.ds((first + j) * TILE, TILE)] = stitched[j]
        psend[pl.ds(first, count)] = jnp.sum(stitched * stitched, axis=1, keepdims=True)
        for k in range(1, strips):
            p_copy(k, i).start()

    for t in range(levels - 1):
        pass_rest(t)
        if t == 0:
            for u in range(levels - 1):
                pass_early(u)
    swap_early()
    hear(0, (z > 0) & jnp.logical_not(high) & (levels > 1))
    hear(1, (z < levels - 1) & jnp.logical_not(low) & (levels > 1))

    for c in range(len(chunks)):
        zsend[z, span(c)] = blocks[z, x, span(c)]
        for level, there in sources():

            @pl.when(there)
            def _():
                z_copy(z, c, z, level).wait_recv()
                zsend[z, span(c)] += zrecv[level, span(c)]

        total = zsend[z, span(c)]
        for k in range(1, lanes):
            x_copy(k, z, c).wait_recv()
            total = total + xrecv[k - 1, z, span(c)]
        settle(1 + c, total)
    total = fkeep[x]
    for k in range(1, lanes):
        g_copy(k).wait_recv()
        total = total + fxrecv[k - 1]
    settle(0, total)

    for i in range(len(parts)):
        for k in range(1, strips):
            p_copy(k, i).wait_recv()
    total = psend[...]
    for k in range(1, strips):
        total = total + precv[k - 1]
    total = total * (1.0 / (strips * height))
    for j in range(tiles):
        power_ref[pl.ds(j, 1), :] = total[j]

    for i in range(len(parts)):
        for k in range(1, strips):
            p_copy(k, i).wait_send()
    for k in range(1, lanes):
        g_copy(k).wait_send()
    for t in range(levels):
        d = dest(t) if t < levels - 1 else z
        for c in range(len(chunks)):
            for k in range(1, lanes):
                x_copy(k, d, c).wait_send()
            if t < levels - 1:
                z_copy(d, c, z, z).wait_send()
        if t < levels - 1:
            f_copy(d, z, z).wait_send()


def finish(stitched_ref, power_ref, out_ref, power_out, sems):
    copies = [
        pltpu.make_async_copy(stitched_ref, out_ref, sems.at[0]),
        pltpu.make_async_copy(power_ref, power_out, sems.at[1]),
    ]
    for copy in copies:
        copy.start()
    for copy in copies:
        copy.wait()


def body(strips, lanes, residuals, corr_rows, corr_cols, row_anchor, col_anchor, first, end, slots):
    local, fh, fw = residuals.shape
    height = fh // 4
    levels = strips // lanes
    others = max(lanes - 1, 1)
    vmem = pl.BlockSpec(memory_space=pltpu.VMEM)
    hbm = pl.BlockSpec(memory_space=pltpu.HBM)
    dma = pltpu.SemaphoreType.DMA
    tiles = fw // TILE
    early = max(round(EARLY * tiles), 1)
    chunks = len(column_chunks(tiles, early))
    block_bytes = 4 * height * fw
    margin = 4 * 1024 * 1024
    blocks = 8 * local + (2 + others) * strips + 5 * levels + 4
    stitched, power = pl.pallas_call(
        functools.partial(kernel, strips, lanes),
        out_shape=(
            jax.ShapeDtypeStruct((height, fw), jnp.float32),
            jax.ShapeDtypeStruct((tiles, TILE), jnp.float32),
        ),
        in_specs=[hbm] * 8,
        out_specs=(vmem, vmem),
        scratch_shapes=[pltpu.SMEM(slots.shape, jnp.int32)] * 5
        + [
            pltpu.VMEM((local, fh, fw), jnp.float32),
            pltpu.VMEM((1, fh), jnp.float32),
            pltpu.VMEM((tiles, TILE), jnp.float32),
            pltpu.VMEM((local, fh, fw), jnp.float32),
            pltpu.VMEM((levels, lanes, tiles, height, TILE), jnp.float32),
            pltpu.VMEM((tiles, height, TILE), jnp.float32),
            pltpu.VMEM((others, levels, tiles, height, TILE), jnp.float32),
            pltpu.VMEM((levels, tiles, height, TILE), jnp.float32),
            pltpu.VMEM((3 * levels, tiles, height, TILE), jnp.float32),
            pltpu.VMEM((levels, lanes, early, height, TILE), jnp.float32),
            pltpu.VMEM((3 * levels, lanes, early, height, TILE), jnp.float32),
            pltpu.VMEM((lanes, early, height, TILE), jnp.float32),
            pltpu.VMEM((others, early, height, TILE), jnp.float32),
            pltpu.VMEM((others, early, height, TILE), jnp.float32),
            pltpu.VMEM((tiles, 1, TILE), jnp.float32),
            pltpu.VMEM((strips - 1, tiles, 1, TILE), jnp.float32),
            pltpu.SemaphoreType.REGULAR((2,)),
            dma((7 + local,)),
            dma((others, levels, chunks)),
            dma((others, levels, chunks)),
            dma((levels, chunks)),
            dma((3 * levels, chunks)),
            dma((levels,)),
            dma((3 * levels,)),
            dma((others,)),
            dma((others,)),
            dma((strips - 1, chunks + 1)),
            dma((strips - 1, chunks + 1)),
        ],
        compiler_params=pltpu.CompilerParams(
            collective_id=0,
            has_side_effects=True,
            vmem_limit_bytes=blocks * block_bytes + margin,
        ),
    )(*(
        pltpu.with_memory_space_constraint(operand, pltpu.HBM)
        for operand in (
            slots, row_anchor, col_anchor, first, end,
            corr_rows[None, :], corr_cols.reshape(fw // TILE, TILE), residuals,
        )
    ))
    stitched, power = pl.pallas_call(
        finish,
        out_shape=(
            jax.ShapeDtypeStruct((height, fw), jnp.float32),
            jax.ShapeDtypeStruct((fw // TILE, TILE), jnp.float32),
        ),
        in_specs=[vmem, vmem],
        out_specs=(hbm, hbm),
        scratch_shapes=[dma((2,))],
    )(*(pltpu.with_memory_space_constraint(part, pltpu.VMEM) for part in (stitched, power)))
    return stitched, power.reshape(fw)


def solution(mesh):
    strips = mesh.shape["strip"]
    lanes = math.gcd(strips, max(mesh.shape["col"] // 2, 1))
    in_specs = (P("strip", None, None), P(), P(), P(), P(), P(), P(), P())
    out_specs = (P("strip", "col"), P("col"))
    run = functools.partial(body, strips, lanes)
    return jax.shard_map(run, mesh=mesh, in_specs=in_specs, out_specs=out_specs, check_vma=False)
```

```python
import functools
import math

import jax
import jax.numpy as jnp
from jax import lax
from jax.experimental import pallas as pl
from jax.experimental.pallas import tpu as pltpu
from jax.sharding import PartitionSpec as P

MESH = pl.DeviceIdType.MESH
CHUNKS = 3
EARLY = 0.15
TILE = 128


def taper(position, count):
    angle = (position.astype(jnp.float32) + (0.5 - count / 2)) * (math.pi / count)
    square = angle * angle
    value = jnp.full_like(square, 1.0 / math.factorial(12))
    for order in (10, 8, 6, 4, 2, 0):
        sign = -1.0 if order % 4 == 2 else 1.0
        value = value * square + sign / math.factorial(order)
    return value * value


def fed(levels, z, d):
    return (z == 1 < d) or (z == levels - 2 > d)


def visit_order(levels):
    return [
        sorted((d for d in range(levels) if d != z), key=lambda d: (fed(levels, z, d), -abs(d - z)))
        for z in range(levels)
    ]


def column_chunks(tiles, first):
    edges = [first + (tiles - first) * c // CHUNKS for c in range(CHUNKS + 1)]
    return [(a, b - a) for a, b in zip(edges, edges[1:]) if b > a]


def kernel(
    strips, lanes,
    slots_hbm, row_hbm, col_hbm, first_hbm, end_hbm, rows_hbm, cols_hbm, res_hbm,
    out_ref, power_ref,
    slots_ref, row_ref, col_ref, first_ref, end_ref, res_ref, rows_ref, cols_ref, turned, blocks, inv, xrecv, zsend, zrecv,
    fsend, frecv, fkeep, fxsend, fxrecv, psend, precv,
    line, in_sem, xs_sem, xr_sem, zs_sem, zr_sem, fs_sem, fr_sem, gs_sem, gr_sem, ps_sem, pr_sem,
):
    local, fh, fw = res_ref.shape
    facets = slots_ref.shape[0]
    height = out_ref.shape[0]
    levels = strips // lanes
    tiles = fw // TILE
    early = fsend.shape[2]
    chunks = column_chunks(tiles, early)
    parts = [(0, early)] + chunks
    strip = lax.axis_index("strip")
    group = lax.axis_index("col")
    z, x = lax.div(strip, lanes), lax.rem(strip, lanes)

    sources = [
        (slots_hbm, slots_ref), (row_hbm, row_ref), (col_hbm, col_ref), (first_hbm, first_ref),
        (end_hbm, end_ref), (rows_hbm, rows_ref), (cols_hbm, cols_ref),
    ]
    small = len(sources)
    sources += [(res_hbm.at[p], res_ref.at[p]) for p in range(local)]
    loads = [
        pltpu.make_async_copy(source, target, in_sem.at[i])
        for i, (source, target) in enumerate(sources)
    ]
    for load in loads:
        load.start()

    low, high = z > 0, z < levels - 1
    leaf = jnp.logical_not(low & high)

    def at(level, lane):
        return {"strip": level * lanes + lane}

    barrier = pltpu.get_barrier_semaphore()
    for k in range(1, lanes):
        pl.semaphore_signal(barrier, device_id=at(z, lax.rem(x + k, lanes)), device_id_type=MESH)
    for there, step in ((low, -1), (high, 1)):

        @pl.when(there)
        def _():
            pl.semaphore_signal(barrier, device_id=at(z + step, x), device_id_type=MESH)

    def enter():
        pl.semaphore_wait(barrier, lanes - 1 + low.astype(jnp.int32) + high.astype(jnp.int32))
        for side, there, step in ((0, jnp.logical_not(low) & high, 1), (1, jnp.logical_not(high) & low, -1)):

            @pl.when(there)
            def _():
                pl.semaphore_signal(line.at[side], device_id=at(z + step, x), device_id_type=MESH)

    def hear(side, when):
        @pl.when(when)
        def _():
            pl.semaphore_wait(line.at[side], 1)

            @pl.when(high if side == 0 else low)
            def _():
                pl.semaphore_signal(
                    line.at[side], device_id=at(z + (1 if side == 0 else -1), x), device_id_type=MESH
                )

    order = visit_order(levels)

    def pick(values):
        value = jnp.int32(values[0])
        for level in range(1, levels):
            value = jnp.where(z == level, jnp.int32(values[level]), value)
        return value

    def dest(t):
        return pick([row[t] for row in order])

    def is_fed(t):
        return pick([int(fed(levels, level, row[t])) for level, row in enumerate(order)]) == 1

    def route(d):
        target = jnp.where(z == 0, min(1, levels - 1), jnp.where(high, d, levels - 2))
        slot = jnp.where(target == d, z, jnp.where(z == 0, levels + d, 2 * levels + d))
        return target, slot

    def inlet(d):
        return jnp.where(d > z, levels + d, 2 * levels + d)

    def sources():
        for level in range(levels):
            if 0 < level < levels - 1:
                yield level, z != level
            elif levels > 1:
                yield level, z == (1 if level == 0 else levels - 2)

    def lane_of(k):
        return lax.rem(x + k, lanes)

    def span(c):
        return pl.ds(chunks[c][0], chunks[c][1])

    def x_copy(k, d, c):
        return pltpu.make_async_remote_copy(
            src_ref=blocks.at[d, lane_of(k), span(c)],
            dst_ref=xrecv.at[k - 1, d, span(c)],
            send_sem=xs_sem.at[k - 1, d, c],
            recv_sem=xr_sem.at[k - 1, d, c],
            device_id=at(z, lane_of(k)),
            device_id_type=MESH,
        )

    def z_copy(d, c, target, slot):
        return pltpu.make_async_remote_copy(
            src_ref=zsend.at[d, span(c)],
            dst_ref=zrecv.at[slot, span(c)],
            send_sem=zs_sem.at[d, c],
            recv_sem=zr_sem.at[slot, c],
            device_id=at(target, x),
            device_id_type=MESH,
        )

    def f_copy(d, target, slot, source=None):
        return pltpu.make_async_remote_copy(
            src_ref=fsend.at[d] if source is None else source,
            dst_ref=frecv.at[slot],
            send_sem=fs_sem.at[d],
            recv_sem=fr_sem.at[slot],
            device_id=at(target, x),
            device_id_type=MESH,
        )

    def g_copy(k):
        return pltpu.make_async_remote_copy(
            src_ref=fxsend.at[k - 1],
            dst_ref=fxrecv.at[k - 1],
            send_sem=gs_sem.at[k - 1],
            recv_sem=gr_sem.at[k - 1],
            device_id=at(z, lane_of(k)),
            device_id_type=MESH,
        )

    def p_copy(k, i):
        return pltpu.make_async_remote_copy(
            src_ref=psend.at[pl.ds(*parts[i])],
            dst_ref=precv.at[k - 1, pl.ds(*parts[i])],
            send_sem=ps_sem.at[k - 1, i],
            recv_sem=pr_sem.at[k - 1, i],
            device_id={"strip": lax.rem(strip + k, strips)},
            device_id_type=MESH,
        )

    eye = lax.broadcasted_iota(jnp.int32, (fh, fh), 0) == lax.broadcasted_iota(
        jnp.int32, (fh, fh), 1
    )
    y = lax.broadcasted_iota(jnp.int32, (fh, 1), 0)
    u = lax.broadcasted_iota(jnp.int32, (1, fw), 1)
    row_taper = taper(y, fh)
    col_taper = taper(u, fw)
    lane = lax.broadcasted_iota(jnp.int32, (fh, TILE), 1)
    sub = lax.broadcasted_iota(jnp.int32, (8, TILE), 0)
    blank = jnp.zeros((fh, TILE), jnp.float32)
    for p in range(local):
        for i in range(tiles + 1):
            turned[p, i] = blank
            turned[p, 2 * tiles + 1 + i] = blank
    for load in loads[:small]:
        load.wait()
    corr_row = jnp.sum(jnp.where(eye, rows_ref[...], 0.0), axis=1, keepdims=True)
    corr_col = jnp.concatenate([cols_ref[pl.ds(i, 1), :] for i in range(tiles)], axis=1)
    col_scale = col_taper * corr_col
    spots = []
    for p in range(local):
        f = slots_ref[strip * local + p]
        ra, ca = row_ref[f], col_ref[f]
        inside = (y >= first_ref[f]) & (y < end_ref[f])
        row_scale = jnp.broadcast_to(jnp.where(inside, row_taper, 0.0) * corr_row, (fh, TILE))
        turn = ca & (TILE - 1)
        base = jnp.clip(group * tiles - (ca >> 7), -tiles, tiles + 1) + tiles + 1
        spots.append((ra & 7, ra >> 3, turn, base))
        loads[small + p].wait()
        for i in range(tiles):
            columns = pl.ds(i * TILE, TILE)
            term = res_ref[p, :, columns] * col_scale[:, i * TILE : (i + 1) * TILE] * row_scale
            turned[p, tiles + 1 + i] = pltpu.roll(term, turn, axis=1)

    def place(j):
        bands = strips * height // 8
        total = [None] * bands
        for p in range(local):
            lift, drop, turn, base = spots[p]
            piece = jnp.where(lane < turn, turned[p, base + (j - 1)], turned[p, base + j])
            zero = jnp.zeros((8, TILE), jnp.float32)
            rows, held = [], zero
            for row in range(0, fh, 8):
                band = pltpu.roll(piece[row : row + 8], lift, axis=0)
                rows.append(jnp.where(sub < lift, held, band))
                held = band
            rows.append(jnp.where(sub < lift, held, 0.0))
            step = 1
            while step <= bands - fh // 8:
                rows = rows + [zero] * min(step, bands - len(rows))
                moved = [zero] * min(step, bands) + rows
                rows = [jnp.where((drop & step) != 0, new, old) for new, old in zip(moved, rows)]
                step *= 2
            total = [band if old is None else old + band for old, band in zip(total, rows)]
        for s in range(strips):
            for i in range(height // 8):
                blocks[s // lanes, s % lanes, j, pl.ds(i * 8, 8), :] = total[s * (height // 8) + i]

    def open_early():
        for t in range(levels - 1):
            d = dest(t)
            target, slot = route(d)

            @pl.when(jnp.logical_not(is_fed(t)))
            def _():
                f_copy(d, target, slot, blocks.at[d, :, pl.ds(0, early)]).start()

    for i, (first, count) in enumerate(parts):
        for j in range(first, first + count):
            place(j)
            if j == first and i == 1:
                enter()
                open_early()
            if j == first and i > 1:
                for k in range(1, lanes):
                    x_copy(k, dest(0), i - 2).start()
    for k in range(1, lanes):
        x_copy(k, dest(0), len(chunks) - 1).start()
    for t in range(1, levels):
        for c in range(len(chunks)):
            for k in range(1, lanes):
                x_copy(k, dest(t) if t < levels - 1 else z, c).start()
    hear(0, (z == 1) & high)
    hear(1, (z == levels - 2) & low)

    v = lax.broadcasted_iota(jnp.int32, (height, 1), 0) + strip * height
    u8 = lax.broadcasted_iota(jnp.int32, (8, fw), 1) + group * fw
    inv[...] = jnp.zeros_like(inv)

    def add_facet(f, carry):
        row_pos = v - row_ref[f]
        row_inside = (row_pos >= first_ref[f]) & (row_pos < end_ref[f])
        row_part = jnp.where(row_inside, taper(row_pos, fh), 0.0)
        col_pos = u8 - col_ref[f]
        col_inside = (col_pos >= 0) & (col_pos < fw)
        col_part = jnp.where(col_inside, taper(col_pos, fw), 0.0)
        for j in range(tiles):
            for row in range(0, height, 8):
                inv[j, pl.ds(row, 8), :] += (
                    row_part[row : row + 8] * col_part[:, j * TILE : (j + 1) * TILE]
                )
        return carry

    lax.fori_loop(0, facets, add_facet, 0)
    inv[...] = 1.0 / jnp.maximum(inv[...], 0.5)
    hear(0, (z > 1) & high)
    hear(1, (z < levels - 2) & low)

    def gather_x(d, c):
        total = blocks[d, x, span(c)]
        for k in range(1, lanes):
            x_copy(k, d, c).wait_recv()
            total = total + xrecv[k - 1, d, span(c)]
        return total

    def pass_early(t):
        d = dest(t)
        target, slot = route(d)

        @pl.when(is_fed(t))
        def _():
            f_copy(d, z, inlet(d)).wait_recv()
            fsend[d] = blocks[d, :, pl.ds(0, early)] + frecv[inlet(d)]
            f_copy(d, target, slot).start()

    def pass_rest(t):
        d = dest(t)
        target, slot = route(d)
        for c in range(len(chunks)):
            zsend[d, span(c)] = gather_x(d, c)

            @pl.when(is_fed(t))
            def _():
                z_copy(d, c, z, inlet(d)).wait_recv()
                zsend[d, span(c)] += zrecv[inlet(d), span(c)]

            z_copy(d, c, target, slot).start()

    def swap_early():
        fkeep[...] = blocks[z, :, pl.ds(0, early)]
        for level, there in sources():

            @pl.when(there)
            def _():
                f_copy(z, z, level).wait_recv()
                fkeep[...] += frecv[level]

        for k in range(1, lanes):
            fxsend[k - 1] = fkeep[lane_of(k)]
        for k in range(1, lanes):
            g_copy(k).start()

    def settle(i, total):
        first, count = parts[i]
        stitched = total * inv[pl.ds(first, count)]
        for j in range(count):
            out_ref[:, pl.ds((first + j) * TILE, TILE)] = stitched[j]
        psend[pl.ds(first, count)] = jnp.sum(stitched * stitched, axis=1, keepdims=True)
        for k in range(1, strips):
            p_copy(k, i).start()

    for t in range(levels - 1):
        pass_rest(t)
        if t == 0:
            for u in range(levels - 1):
                pass_early(u)
    swap_early()
    hear(0, (z > 0) & jnp.logical_not(high) & (levels > 1))
    hear(1, (z < levels - 1) & jnp.logical_not(low) & (levels > 1))

    for c in range(len(chunks)):
        zsend[z, span(c)] = blocks[z, x, span(c)]
        for level, there in sources():

            @pl.when(there)
            def _():
                z_copy(z, c, z, level).wait_recv()
                zsend[z, span(c)] += zrecv[level, span(c)]

        total = zsend[z, span(c)]
        for k in range(1, lanes):
            x_copy(k, z, c).wait_recv()
            total = total + xrecv[k - 1, z, span(c)]
        settle(1 + c, total)
    total = fkeep[x]
    for k in range(1, lanes):
        g_copy(k).wait_recv()
        total = total + fxrecv[k - 1]
    settle(0, total)

    for i in range(len(parts)):
        for k in range(1, strips):
            p_copy(k, i).wait_send()
    for k in range(1, lanes):
        g_copy(k).wait_send()
    for t in range(levels):
        d = dest(t) if t < levels - 1 else z
        for c in range(len(chunks)):
            for k in range(1, lanes):
                x_copy(k, d, c).wait_send()
            if t < levels - 1:
                z_copy(d, c, z, z).wait_send()
        if t < levels - 1:
            f_copy(d, z, z).wait_send()

    for i in range(len(parts)):
        for k in range(1, strips):
            p_copy(k, i).wait_recv()
    total = psend[...]
    for k in range(1, strips):
        total = total + precv[k - 1]
    total = total * (1.0 / (strips * height))
    for j in range(tiles):
        power_ref[pl.ds(j, 1), :] = total[j]


def finish(stitched_ref, power_ref, out_ref, power_out, sems):
    copies = [
        pltpu.make_async_copy(stitched_ref, out_ref, sems.at[0]),
        pltpu.make_async_copy(power_ref, power_out, sems.at[1]),
    ]
    for copy in copies:
        copy.start()
    for copy in copies:
        copy.wait()


def body(strips, lanes, residuals, corr_rows, corr_cols, row_anchor, col_anchor, first, end, slots):
    local, fh, fw = residuals.shape
    height = fh // 4
    levels = strips // lanes
    others = max(lanes - 1, 1)
    vmem = pl.BlockSpec(memory_space=pltpu.VMEM)
    hbm = pl.BlockSpec(memory_space=pltpu.HBM)
    dma = pltpu.SemaphoreType.DMA
    tiles = fw // TILE
    early = max(round(EARLY * tiles), 1)
    chunks = len(column_chunks(tiles, early))
    block_bytes = 4 * height * fw
    margin = 4 * 1024 * 1024
    blocks = 18 * local + (2 + others) * strips + 5 * levels + 4
    stitched, power = pl.pallas_call(
        functools.partial(kernel, strips, lanes),
        out_shape=(
            jax.ShapeDtypeStruct((height, fw), jnp.float32),
            jax.ShapeDtypeStruct((tiles, TILE), jnp.float32),
        ),
        in_specs=[hbm] * 8,
        out_specs=(vmem, vmem),
        scratch_shapes=[pltpu.SMEM(slots.shape, jnp.int32)] * 5
        + [
            pltpu.VMEM((local, fh, fw), jnp.float32),
            pltpu.VMEM((1, fh), jnp.float32),
            pltpu.VMEM((tiles, TILE), jnp.float32),
            pltpu.VMEM((local, 3 * tiles + 2, fh, TILE), jnp.float32),
            pltpu.VMEM((levels, lanes, tiles, height, TILE), jnp.float32),
            pltpu.VMEM((tiles, height, TILE), jnp.float32),
            pltpu.VMEM((others, levels, tiles, height, TILE), jnp.float32),
            pltpu.VMEM((levels, tiles, height, TILE), jnp.float32),
            pltpu.VMEM((3 * levels, tiles, height, TILE), jnp.float32),
            pltpu.VMEM((levels, lanes, early, height, TILE), jnp.float32),
            pltpu.VMEM((3 * levels, lanes, early, height, TILE), jnp.float32),
            pltpu.VMEM((lanes, early, height, TILE), jnp.float32),
            pltpu.VMEM((others, early, height, TILE), jnp.float32),
            pltpu.VMEM((others, early, height, TILE), jnp.float32),
            pltpu.VMEM((tiles, 1, TILE), jnp.float32),
            pltpu.VMEM((strips - 1, tiles, 1, TILE), jnp.float32),
            pltpu.SemaphoreType.REGULAR((2,)),
            dma((7 + local,)),
            dma((others, levels, chunks)),
            dma((others, levels, chunks)),
            dma((levels, chunks)),
            dma((3 * levels, chunks)),
            dma((levels,)),
            dma((3 * levels,)),
            dma((others,)),
            dma((others,)),
            dma((strips - 1, chunks + 1)),
            dma((strips - 1, chunks + 1)),
        ],
        compiler_params=pltpu.CompilerParams(
            collective_id=0,
            has_side_effects=True,
            vmem_limit_bytes=blocks * block_bytes + margin,
        ),
    )(*(
        pltpu.with_memory_space_constraint(operand, pltpu.HBM)
        for operand in (
            slots, row_anchor, col_anchor, first, end,
            corr_rows[None, :], corr_cols.reshape(fw // TILE, TILE), residuals,
        )
    ))
    stitched, power = pl.pallas_call(
        finish,
        out_shape=(
            jax.ShapeDtypeStruct((height, fw), jnp.float32),
            jax.ShapeDtypeStruct((fw // TILE, TILE), jnp.float32),
        ),
        in_specs=[vmem, vmem],
        out_specs=(hbm, hbm),
        scratch_shapes=[dma((2,))],
    )(*(pltpu.with_memory_space_constraint(part, pltpu.VMEM) for part in (stitched, power)))
    return stitched, power.reshape(fw)


def solution(mesh):
    strips = mesh.shape["strip"]
    lanes = math.gcd(strips, max(mesh.shape["col"] // 2, 1))
    in_specs = (P("strip", None, None), P(), P(), P(), P(), P(), P(), P())
    out_specs = (P("strip", "col"), P("col"))
    run = functools.partial(body, strips, lanes)
    return jax.shard_map(run, mesh=mesh, in_specs=in_specs, out_specs=out_specs, check_vma=False)
```

```python
import functools
import math

import jax
import jax.numpy as jnp
from jax import lax
from jax.experimental import pallas as pl
from jax.experimental.pallas import tpu as pltpu
from jax.sharding import PartitionSpec as P

MESH = pl.DeviceIdType.MESH
SHARES = (5, 6, 6)
EARLY = 0.15
TILE = 128


def taper(position, count):
    angle = (position.astype(jnp.float32) + (0.5 - count / 2)) * (math.pi / count)
    square = angle * angle
    value = jnp.full_like(square, 1.0 / math.factorial(12))
    for order in (10, 8, 6, 4, 2, 0):
        sign = -1.0 if order % 4 == 2 else 1.0
        value = value * square + sign / math.factorial(order)
    return value * value


def fed(levels, z, d):
    return (z == 1 < d) or (z == levels - 2 > d)


def visit_order(levels):
    return [
        sorted((d for d in range(levels) if d != z), key=lambda d: (fed(levels, z, d), -abs(d - z)))
        for z in range(levels)
    ]


def inlets(levels):
    def inner(level):
        return 0 < level < levels - 1

    tables = []
    for z in range(levels):
        passed = [("pass", d) for d in range(levels) if d != z and fed(levels, z, d)]
        direct = [
            ("sum", s) for s in range(levels)
            if s != z and (inner(s) or (z == (1 if s == 0 else levels - 2)))
        ]
        tables.append(passed + direct)
    return tables


def column_chunks(tiles, first):
    ends = [sum(SHARES[:c]) for c in range(len(SHARES) + 1)]
    edges = [first + (tiles - first) * end // ends[-1] for end in ends]
    return [(a, b - a) for a, b in zip(edges, edges[1:]) if b > a]


def kernel(
    strips, lanes,
    slots_hbm, row_hbm, col_hbm, first_hbm, end_hbm, rows_hbm, cols_hbm, res_hbm,
    out_ref, power_ref,
    slots_ref, row_ref, col_ref, first_ref, end_ref, res_ref, rows_ref, cols_ref, turned, blocks, inv, xrecv, zsend, zrecv,
    fsend, frecv, fkeep, fxsend, fxrecv, psend, precv,
    line, in_sem, sent, xr_sem, zr_sem, fr_sem, gr_sem, pr_sem,
):
    local, fh, fw = res_ref.shape
    facets = slots_ref.shape[0]
    height = out_ref.shape[0]
    levels = strips // lanes
    tiles = fw // TILE
    early = fsend.shape[2]
    chunks = column_chunks(tiles, early)
    parts = [(0, early)] + chunks
    strip = lax.axis_index("strip")
    group = lax.axis_index("col")
    z, x = lax.div(strip, lanes), lax.rem(strip, lanes)

    sources = [
        (slots_hbm, slots_ref), (row_hbm, row_ref), (col_hbm, col_ref), (first_hbm, first_ref),
        (end_hbm, end_ref), (rows_hbm, rows_ref), (cols_hbm, cols_ref),
    ]
    small = len(sources)
    sources += [(res_hbm.at[p], res_ref.at[p]) for p in range(local)]
    loads = [
        pltpu.make_async_copy(source, target, in_sem.at[i])
        for i, (source, target) in enumerate(sources)
    ]
    for load in loads:
        load.start()

    low, high = z > 0, z < levels - 1
    leaf = jnp.logical_not(low & high)

    def at(level, lane):
        return {"strip": level * lanes + lane}

    barrier = pltpu.get_barrier_semaphore()
    for k in range(1, lanes):
        pl.semaphore_signal(barrier, device_id=at(z, lax.rem(x + k, lanes)), device_id_type=MESH)
    for there, step in ((low, -1), (high, 1)):

        @pl.when(there)
        def _():
            pl.semaphore_signal(barrier, device_id=at(z + step, x), device_id_type=MESH)

    def enter():
        pl.semaphore_wait(barrier, lanes - 1 + low.astype(jnp.int32) + high.astype(jnp.int32))
        for side, there, step in ((0, jnp.logical_not(low) & high, 1), (1, jnp.logical_not(high) & low, -1)):

            @pl.when(there)
            def _():
                pl.semaphore_signal(line.at[side], device_id=at(z + step, x), device_id_type=MESH)

    def hear(side, when):
        @pl.when(when)
        def _():
            pl.semaphore_wait(line.at[side], 1)

            @pl.when(high if side == 0 else low)
            def _():
                pl.semaphore_signal(
                    line.at[side], device_id=at(z + (1 if side == 0 else -1), x), device_id_type=MESH
                )

    order = visit_order(levels)

    def pick(values):
        value = jnp.int32(values[0])
        for level in range(1, levels):
            value = jnp.where(z == level, jnp.int32(values[level]), value)
        return value

    def dest(t):
        return pick([row[t] for row in order])

    def is_fed(t):
        return pick([int(fed(levels, level, row[t])) for level, row in enumerate(order)]) == 1

    tables = inlets(levels)
    leaves = {0: min(1, levels - 1), levels - 1: max(levels - 2, 0)}

    def route(t):
        targets, slots = [], []
        for level, row in enumerate(order):
            target = leaves.get(level, row[t])
            kind = ("sum", level) if target == row[t] else ("pass", row[t])
            targets.append(target)
            slots.append(tables[target].index(kind))
        return pick(targets), pick(slots)

    def inlet(t):
        return pick([
            tables[level].index(("pass", row[t])) if fed(levels, level, row[t]) else 0
            for level, row in enumerate(order)
        ])

    def sources():
        for i in range(max(len(table) for table in tables)):
            which = [i < len(table) and table[i][0] == "sum" for table in tables]
            if any(which):
                yield i, pick([int(there) for there in which]) == 1

    def lane_of(k):
        return lax.rem(x + k, lanes)

    def span(c):
        return pl.ds(chunks[c][0], chunks[c][1])

    def x_copy(k, d, c):
        return pltpu.make_async_remote_copy(
            src_ref=blocks.at[d, lane_of(k), span(c)],
            dst_ref=xrecv.at[k - 1, d, span(c)],
            send_sem=sent.at[0],
            recv_sem=xr_sem.at[k - 1, d, c],
            device_id=at(z, lane_of(k)),
            device_id_type=MESH,
        )

    def z_copy(d, c, target, slot):
        return pltpu.make_async_remote_copy(
            src_ref=zsend.at[d, span(c)],
            dst_ref=zrecv.at[slot, span(c)],
            send_sem=sent.at[1],
            recv_sem=zr_sem.at[slot, c],
            device_id=at(target, x),
            device_id_type=MESH,
        )

    def f_copy(d, target, slot, source=None):
        return pltpu.make_async_remote_copy(
            src_ref=fsend.at[d] if source is None else source,
            dst_ref=frecv.at[slot],
            send_sem=sent.at[2],
            recv_sem=fr_sem.at[slot],
            device_id=at(target, x),
            device_id_type=MESH,
        )

    def g_copy(k):
        return pltpu.make_async_remote_copy(
            src_ref=fxsend.at[k - 1],
            dst_ref=fxrecv.at[k - 1],
            send_sem=sent.at[3],
            recv_sem=gr_sem.at[k - 1],
            device_id=at(z, lane_of(k)),
            device_id_type=MESH,
        )

    def p_copy(k, i):
        return pltpu.make_async_remote_copy(
            src_ref=psend.at[pl.ds(*parts[i])],
            dst_ref=precv.at[k - 1, pl.ds(*parts[i])],
            send_sem=sent.at[4],
            recv_sem=pr_sem.at[i],
            device_id={"strip": lax.rem(strip + k, strips)},
            device_id_type=MESH,
        )

    eye = lax.broadcasted_iota(jnp.int32, (fh, fh), 0) == lax.broadcasted_iota(
        jnp.int32, (fh, fh), 1
    )
    y = lax.broadcasted_iota(jnp.int32, (fh, 1), 0)
    u = lax.broadcasted_iota(jnp.int32, (1, fw), 1)
    row_taper = taper(y, fh)
    col_taper = taper(u, fw)
    lane = lax.broadcasted_iota(jnp.int32, (fh, TILE), 1)
    sub = lax.broadcasted_iota(jnp.int32, (8, TILE), 0)
    blank = jnp.zeros((fh, TILE), jnp.float32)
    for p in range(local):
        for i in range(tiles + 1):
            turned[p, i] = blank
            turned[p, 2 * tiles + 1 + i] = blank
    for load in loads[:small]:
        load.wait()
    corr_row = jnp.sum(jnp.where(eye, rows_ref[...], 0.0), axis=1, keepdims=True)
    corr_col = jnp.concatenate([cols_ref[pl.ds(i, 1), :] for i in range(tiles)], axis=1)
    col_scale = col_taper * corr_col
    spots = []
    for p in range(local):
        f = slots_ref[strip * local + p]
        ra, ca = row_ref[f], col_ref[f]
        inside = (y >= first_ref[f]) & (y < end_ref[f])
        row_scale = jnp.broadcast_to(jnp.where(inside, row_taper, 0.0) * corr_row, (fh, TILE))
        turn = ca & (TILE - 1)
        base = jnp.clip(group * tiles - (ca >> 7), -tiles, tiles + 1) + tiles + 1
        spots.append((ra & 7, ra >> 3, turn, base))
        loads[small + p].wait()
        for i in range(tiles):
            columns = pl.ds(i * TILE, TILE)
            term = res_ref[p, :, columns] * col_scale[:, i * TILE : (i + 1) * TILE] * row_scale
            turned[p, tiles + 1 + i] = pltpu.roll(term, turn, axis=1)

    def place(j):
        bands = strips * height // 8
        total = [None] * bands
        for p in range(local):
            lift, drop, turn, base = spots[p]
            piece = jnp.where(lane < turn, turned[p, base + (j - 1)], turned[p, base + j])
            zero = jnp.zeros((8, TILE), jnp.float32)
            rows, held = [], zero
            for row in range(0, fh, 8):
                band = pltpu.roll(piece[row : row + 8], lift, axis=0)
                rows.append(jnp.where(sub < lift, held, band))
                held = band
            rows.append(jnp.where(sub < lift, held, 0.0))
            step = 1
            while step <= bands - fh // 8:
                rows = rows + [zero] * min(step, bands - len(rows))
                moved = [zero] * min(step, bands) + rows
                rows = [jnp.where((drop & step) != 0, new, old) for new, old in zip(moved, rows)]
                step *= 2
            total = [band if old is None else old + band for old, band in zip(total, rows)]
        for s in range(strips):
            for i in range(height // 8):
                blocks[s // lanes, s % lanes, j, pl.ds(i * 8, 8), :] = total[s * (height // 8) + i]

    def open_early():
        for t in range(levels - 1):
            d = dest(t)
            target, slot = route(t)

            @pl.when(jnp.logical_not(is_fed(t)))
            def _():
                f_copy(d, target, slot, blocks.at[d, :, pl.ds(0, early)]).start()

    def open_chunk(c):
        @pl.when(lax.rem(group, 2) == 0)
        def _():
            for k in range(1, lanes):
                x_copy(k, dest(0), c).start()

    openers = [lambda: open_chunk(0), open_early] + [
        functools.partial(open_chunk, c) for c in range(1, len(chunks))
    ]
    for i, (first, count) in enumerate([chunks[0], parts[0]] + chunks[1:]):
        for j in range(first, first + count):
            place(j)
            if j == first and i == 1:
                enter()
            if j == first and i > 0:
                openers[i - 1]()
    openers[-1]()

    @pl.when(lax.rem(group, 2) == 0)
    def _():
        for t in range(1, levels):
            for c in range(len(chunks)):
                for k in range(1, lanes):
                    x_copy(k, dest(t) if t < levels - 1 else z, c).start()

    hear(0, (z == 1) & high)
    hear(1, (z == levels - 2) & low)

    v = lax.broadcasted_iota(jnp.int32, (height, 1), 0) + strip * height
    u8 = lax.broadcasted_iota(jnp.int32, (8, fw), 1) + group * fw
    inv[...] = jnp.zeros_like(inv)

    def add_facet(f, carry):
        row_pos = v - row_ref[f]
        row_inside = (row_pos >= first_ref[f]) & (row_pos < end_ref[f])
        row_part = jnp.where(row_inside, taper(row_pos, fh), 0.0)
        col_pos = u8 - col_ref[f]
        col_inside = (col_pos >= 0) & (col_pos < fw)
        col_part = jnp.where(col_inside, taper(col_pos, fw), 0.0)
        for j in range(tiles):
            for row in range(0, height, 8):
                inv[j, pl.ds(row, 8), :] += (
                    row_part[row : row + 8] * col_part[:, j * TILE : (j + 1) * TILE]
                )
        return carry

    lax.fori_loop(0, facets, add_facet, 0)
    inv[...] = 1.0 / jnp.maximum(inv[...], 0.5)

    @pl.when(lax.rem(group, 2) == 1)
    def _():
        for t in range(0, levels):
            for c in range(len(chunks)):
                for k in range(1, lanes):
                    x_copy(k, dest(t) if t < levels - 1 else z, c).start()

    hear(0, (z > 1) & high)
    hear(1, (z < levels - 2) & low)

    def gather_x(d, c):
        total = blocks[d, x, span(c)]
        for k in range(1, lanes):
            x_copy(k, d, c).wait_recv()
            total = total + xrecv[k - 1, d, span(c)]
        return total

    def pass_early(t):
        d = dest(t)
        target, slot = route(t)

        @pl.when(is_fed(t))
        def _():
            f_copy(d, z, inlet(t)).wait_recv()
            fsend[d] = blocks[d, :, pl.ds(0, early)] + frecv[inlet(t)]
            f_copy(d, target, slot).start()

    def pass_rest(t):
        d = dest(t)
        target, slot = route(t)
        for c in range(len(chunks)):
            zsend[d, span(c)] = gather_x(d, c)

            @pl.when(is_fed(t))
            def _():
                z_copy(d, c, z, inlet(t)).wait_recv()
                zsend[d, span(c)] += zrecv[inlet(t), span(c)]

            z_copy(d, c, target, slot).start()

    def swap_early():
        fkeep[...] = blocks[z, :, pl.ds(0, early)]
        for level, there in sources():

            @pl.when(there)
            def _():
                f_copy(z, z, level).wait_recv()
                fkeep[...] += frecv[level]

        for k in range(1, lanes):
            fxsend[k - 1] = fkeep[lane_of(k)]
        for k in range(1, lanes):
            g_copy(k).start()

    def settle(i, total):
        first, count = parts[i]
        stitched = total * inv[pl.ds(first, count)]
        for j in range(count):
            out_ref[:, pl.ds((first + j) * TILE, TILE)] = stitched[j]
        psend[pl.ds(first, count)] = jnp.sum(stitched * stitched, axis=1, keepdims=True)
        for k in range(1, strips):
            p_copy(k, i).start()

    for t in range(levels - 1):
        pass_rest(t)
        if t == 0:
            for u in range(levels - 1):
                pass_early(u)
    swap_early()
    hear(0, (z > 0) & jnp.logical_not(high) & (levels > 1))
    hear(1, (z < levels - 1) & jnp.logical_not(low) & (levels > 1))

    for c in range(len(chunks)):
        zsend[z, span(c)] = blocks[z, x, span(c)]
        for level, there in sources():

            @pl.when(there)
            def _():
                z_copy(z, c, z, level).wait_recv()
                zsend[z, span(c)] += zrecv[level, span(c)]

        total = zsend[z, span(c)]
        for k in range(1, lanes):
            x_copy(k, z, c).wait_recv()
            total = total + xrecv[k - 1, z, span(c)]
        settle(1 + c, total)
    total = fkeep[x]
    for k in range(1, lanes):
        g_copy(k).wait_recv()
        total = total + fxrecv[k - 1]
    settle(0, total)

    def drain(i, ref):
        pltpu.make_async_remote_copy(
            src_ref=ref, dst_ref=ref, send_sem=sent.at[i], recv_sem=sent.at[i],
            device_id=at(z, x), device_id_type=MESH,
        ).wait_send()

    rest = pl.ds(early, tiles - early)
    if lanes > 1:
        drain(0, xrecv.at[:, :, rest])
        drain(3, fxsend)
    if levels > 1:
        drain(1, zsend.at[pl.ds(0, levels - 1), rest])
        drain(2, fsend.at[pl.ds(0, levels - 1)])
    if strips > 1:
        drain(4, precv)

    for i in list(range(1, len(parts))) + [0]:
        first, count = parts[i]
        if strips > 1:
            came = precv.at[:, pl.ds(first, count)]
            pltpu.make_async_remote_copy(
                src_ref=came, dst_ref=came, send_sem=sent.at[4], recv_sem=pr_sem.at[i],
                device_id=at(z, x), device_id_type=MESH,
            ).wait_recv()
        total = psend[pl.ds(first, count)]
        for k in range(1, strips):
            total = total + precv[k - 1, pl.ds(first, count)]
        total = total * (1.0 / (strips * height))
        for j in range(count):
            power_ref[pl.ds(first + j, 1), :] = total[j]


def finish(stitched_ref, power_ref, out_ref, power_out, sems):
    copies = [
        pltpu.make_async_copy(stitched_ref, out_ref, sems.at[0]),
        pltpu.make_async_copy(power_ref, power_out, sems.at[1]),
    ]
    for copy in copies:
        copy.start()
    for copy in copies:
        copy.wait()


def body(strips, lanes, residuals, corr_rows, corr_cols, row_anchor, col_anchor, first, end, slots):
    local, fh, fw = residuals.shape
    height = fh // 4
    levels = strips // lanes
    others = max(lanes - 1, 1)
    vmem = pl.BlockSpec(memory_space=pltpu.VMEM)
    hbm = pl.BlockSpec(memory_space=pltpu.HBM)
    dma = pltpu.SemaphoreType.DMA
    tiles = fw // TILE
    early = max(round(EARLY * tiles), 1)
    chunks = len(column_chunks(tiles, early))
    slots_in = max([len(table) for table in inlets(levels)] + [1])
    block_bytes = 4 * height * fw
    margin = 4 * 1024 * 1024
    blocks = 18 * local + (2 + others) * strips + 5 * levels + 4
    stitched, power = pl.pallas_call(
        functools.partial(kernel, strips, lanes),
        out_shape=(
            jax.ShapeDtypeStruct((height, fw), jnp.float32),
            jax.ShapeDtypeStruct((tiles, TILE), jnp.float32),
        ),
        in_specs=[hbm] * 8,
        out_specs=(vmem, vmem),
        scratch_shapes=[pltpu.SMEM(slots.shape, jnp.int32)] * 5
        + [
            pltpu.VMEM((local, fh, fw), jnp.float32),
            pltpu.VMEM((1, fh), jnp.float32),
            pltpu.VMEM((tiles, TILE), jnp.float32),
            pltpu.VMEM((local, 3 * tiles + 2, fh, TILE), jnp.float32),
            pltpu.VMEM((levels, lanes, tiles, height, TILE), jnp.float32),
            pltpu.VMEM((tiles, height, TILE), jnp.float32),
            pltpu.VMEM((others, levels, tiles, height, TILE), jnp.float32),
            pltpu.VMEM((levels, tiles, height, TILE), jnp.float32),
            pltpu.VMEM((slots_in, tiles, height, TILE), jnp.float32),
            pltpu.VMEM((levels, lanes, early, height, TILE), jnp.float32),
            pltpu.VMEM((slots_in, lanes, early, height, TILE), jnp.float32),
            pltpu.VMEM((lanes, early, height, TILE), jnp.float32),
            pltpu.VMEM((others, early, height, TILE), jnp.float32),
            pltpu.VMEM((others, early, height, TILE), jnp.float32),
            pltpu.VMEM((tiles, 1, TILE), jnp.float32),
            pltpu.VMEM((strips - 1, tiles, 1, TILE), jnp.float32),
            pltpu.SemaphoreType.REGULAR((2,)),
            dma((7 + local,)),
            dma((5,)),
            dma((others, levels, chunks)),
            dma((slots_in, chunks)),
            dma((slots_in,)),
            dma((others,)),
            dma((chunks + 1,)),
        ],
        compiler_params=pltpu.CompilerParams(
            collective_id=0,
            has_side_effects=True,
            vmem_limit_bytes=blocks * block_bytes + margin,
        ),
    )(*(
        pltpu.with_memory_space_constraint(operand, pltpu.HBM)
        for operand in (
            slots, row_anchor, col_anchor, first, end,
            corr_rows[None, :], corr_cols.reshape(fw // TILE, TILE), residuals,
        )
    ))
    stitched, power = pl.pallas_call(
        finish,
        out_shape=(
            jax.ShapeDtypeStruct((height, fw), jnp.float32),
            jax.ShapeDtypeStruct((fw // TILE, TILE), jnp.float32),
        ),
        in_specs=[vmem, vmem],
        out_specs=(hbm, hbm),
        scratch_shapes=[dma((2,))],
    )(*(pltpu.with_memory_space_constraint(part, pltpu.VMEM) for part in (stitched, power)))
    return stitched, power.reshape(fw)


def solution(mesh):
    strips = mesh.shape["strip"]
    lanes = math.gcd(strips, max(mesh.shape["col"] // 2, 1))
    in_specs = (P("strip", None, None), P(), P(), P(), P(), P(), P(), P())
    out_specs = (P("strip", "col"), P("col"))
    run = functools.partial(body, strips, lanes)
    return jax.shard_map(run, mesh=mesh, in_specs=in_specs, out_specs=out_specs, check_vma=False)
```

```python
import functools
import math

import jax
import jax.numpy as jnp
from jax import lax
from jax.experimental import pallas as pl
from jax.experimental.pallas import tpu as pltpu
from jax.sharding import PartitionSpec as P

MESH = pl.DeviceIdType.MESH
SHARES = (5, 6, 6)
EARLY = 0.15
TILE = 128


def taper(position, count):
    angle = (position.astype(jnp.float32) + (0.5 - count / 2)) * (math.pi / count)
    square = angle * angle
    value = jnp.full_like(square, 1.0 / math.factorial(12))
    for order in (10, 8, 6, 4, 2, 0):
        sign = -1.0 if order % 4 == 2 else 1.0
        value = value * square + sign / math.factorial(order)
    return value * value


def fed(levels, z, d):
    return (z == 1 < d) or (z == levels - 2 > d)


def visit_order(levels):
    return [
        sorted((d for d in range(levels) if d != z), key=lambda d: (fed(levels, z, d), -abs(d - z)))
        for z in range(levels)
    ]


def inlets(levels):
    def inner(level):
        return 0 < level < levels - 1

    tables = []
    for z in range(levels):
        passed = [("pass", d) for d in range(levels) if d != z and fed(levels, z, d)]
        direct = [
            ("sum", s) for s in range(levels)
            if s != z and (inner(s) or (z == (1 if s == 0 else levels - 2)))
        ]
        tables.append(passed + direct)
    return tables


def column_chunks(tiles, first):
    ends = [sum(SHARES[:c]) for c in range(len(SHARES) + 1)]
    edges = [first + (tiles - first) * end // ends[-1] for end in ends]
    return [(a, b - a) for a, b in zip(edges, edges[1:]) if b > a]


def kernel(
    strips, lanes,
    slots_hbm, row_hbm, col_hbm, first_hbm, end_hbm, rows_hbm, cols_hbm, res_hbm,
    out_ref, power_ref,
    slots_ref, row_ref, col_ref, first_ref, end_ref, rows_ref, cols_ref, scale, turned, blocks, inv, xrecv, zsend, zrecv,
    fsend, frecv, fkeep, fxsend, fxrecv, psend, precv,
    line, sent, xr_sem, zr_sem, fr_sem, gr_sem, pr_sem,
):
    local, fh, fw = res_hbm.shape
    facets = slots_ref.shape[0]
    height = out_ref.shape[0]
    levels = strips // lanes
    tiles = fw // TILE
    early = fsend.shape[2]
    chunks = column_chunks(tiles, early)
    parts = [(0, early)] + chunks
    strip = lax.axis_index("strip")
    group = lax.axis_index("col")
    z, x = lax.div(strip, lanes), lax.rem(strip, lanes)

    low, high = z > 0, z < levels - 1
    leaf = jnp.logical_not(low & high)

    def at(level, lane):
        return {"strip": level * lanes + lane}

    barrier = pltpu.get_barrier_semaphore()
    for k in range(1, lanes):
        pl.semaphore_signal(barrier, device_id=at(z, lax.rem(x + k, lanes)), device_id_type=MESH)
    for there, step in ((low, -1), (high, 1)):

        @pl.when(there)
        def _():
            pl.semaphore_signal(barrier, device_id=at(z + step, x), device_id_type=MESH)

    sources = [
        (slots_hbm, slots_ref), (row_hbm, row_ref), (col_hbm, col_ref), (first_hbm, first_ref),
        (end_hbm, end_ref), (rows_hbm, rows_ref), (cols_hbm, cols_ref),
    ]
    small = len(sources)
    loads = [
        pltpu.make_async_copy(source, target, sent.at[i])
        for i, (source, target) in enumerate(sources)
    ]
    for load in loads:
        load.start()
    for p in range(local):
        for i in range(tiles):
            pltpu.make_async_copy(
                res_hbm.at[p, :, pl.ds(i * TILE, TILE)], turned.at[p, tiles + 1 + i], sent.at[small + p]
            ).start()

    def enter():
        pl.semaphore_wait(barrier, lanes - 1 + low.astype(jnp.int32) + high.astype(jnp.int32))
        for side, there, step in ((0, jnp.logical_not(low) & high, 1), (1, jnp.logical_not(high) & low, -1)):

            @pl.when(there)
            def _():
                pl.semaphore_signal(line.at[side], device_id=at(z + step, x), device_id_type=MESH)

    def hear(side, when):
        @pl.when(when)
        def _():
            pl.semaphore_wait(line.at[side], 1)

            @pl.when(high if side == 0 else low)
            def _():
                pl.semaphore_signal(
                    line.at[side], device_id=at(z + (1 if side == 0 else -1), x), device_id_type=MESH
                )

    order = visit_order(levels)

    def pick(values):
        value = jnp.int32(values[0])
        for level in range(1, levels):
            value = jnp.where(z == level, jnp.int32(values[level]), value)
        return value

    def dest(t):
        return pick([row[t] for row in order])

    def is_fed(t):
        return pick([int(fed(levels, level, row[t])) for level, row in enumerate(order)]) == 1

    tables = inlets(levels)
    leaves = {0: min(1, levels - 1), levels - 1: max(levels - 2, 0)}

    def route(t):
        targets, slots = [], []
        for level, row in enumerate(order):
            target = leaves.get(level, row[t])
            kind = ("sum", level) if target == row[t] else ("pass", row[t])
            targets.append(target)
            slots.append(tables[target].index(kind))
        return pick(targets), pick(slots)

    def inlet(t):
        return pick([
            tables[level].index(("pass", row[t])) if fed(levels, level, row[t]) else 0
            for level, row in enumerate(order)
        ])

    def sources():
        for i in range(max(len(table) for table in tables)):
            which = [i < len(table) and table[i][0] == "sum" for table in tables]
            if any(which):
                yield i, pick([int(there) for there in which]) == 1

    def lane_of(k):
        return lax.rem(x + k, lanes)

    def span(c):
        return pl.ds(chunks[c][0], chunks[c][1])

    def x_copy(k, d, c):
        return pltpu.make_async_remote_copy(
            src_ref=blocks.at[d, lane_of(k), span(c)],
            dst_ref=xrecv.at[k - 1, d, span(c)],
            send_sem=sent.at[0],
            recv_sem=xr_sem.at[k - 1, d, c],
            device_id=at(z, lane_of(k)),
            device_id_type=MESH,
        )

    def z_copy(d, c, target, slot):
        return pltpu.make_async_remote_copy(
            src_ref=zsend.at[d, span(c)],
            dst_ref=zrecv.at[slot, span(c)],
            send_sem=sent.at[1],
            recv_sem=zr_sem.at[slot, c],
            device_id=at(target, x),
            device_id_type=MESH,
        )

    def f_copy(d, target, slot, source=None):
        return pltpu.make_async_remote_copy(
            src_ref=fsend.at[d] if source is None else source,
            dst_ref=frecv.at[slot],
            send_sem=sent.at[2],
            recv_sem=fr_sem.at[slot],
            device_id=at(target, x),
            device_id_type=MESH,
        )

    def g_copy(k):
        return pltpu.make_async_remote_copy(
            src_ref=fxsend.at[k - 1],
            dst_ref=fxrecv.at[k - 1],
            send_sem=sent.at[3],
            recv_sem=gr_sem.at[k - 1],
            device_id=at(z, lane_of(k)),
            device_id_type=MESH,
        )

    def p_copy(k, i):
        return pltpu.make_async_remote_copy(
            src_ref=psend.at[pl.ds(*parts[i])],
            dst_ref=precv.at[k - 1, pl.ds(*parts[i])],
            send_sem=sent.at[4],
            recv_sem=pr_sem.at[i],
            device_id={"strip": lax.rem(strip + k, strips)},
            device_id_type=MESH,
        )

    eye = lax.broadcasted_iota(jnp.int32, (fh, fh), 0) == lax.broadcasted_iota(
        jnp.int32, (fh, fh), 1
    )
    y = lax.broadcasted_iota(jnp.int32, (fh, 1), 0)
    u = lax.broadcasted_iota(jnp.int32, (1, fw), 1)
    row_taper = taper(y, fh)
    col_taper = taper(u, fw)
    lane = lax.broadcasted_iota(jnp.int32, (fh, TILE), 1)
    sub = lax.broadcasted_iota(jnp.int32, (8, TILE), 0)
    blank = jnp.zeros((fh, TILE), jnp.float32)
    for p in range(local):
        for i in range(tiles + 1):
            turned[p, i] = blank
            turned[p, 2 * tiles + 1 + i] = blank
    for load in loads:
        load.wait()
    corr_row = jnp.sum(jnp.where(eye, rows_ref[...], 0.0), axis=1, keepdims=True)
    for i in range(tiles):
        columns = slice(i * TILE, (i + 1) * TILE)
        scale[i] = col_taper[:, columns] * cols_ref[pl.ds(i, 1), :]
    spots = []
    for p in range(local):
        f = slots_ref[strip * local + p]
        ra, ca = row_ref[f], col_ref[f]
        inside = (y >= first_ref[f]) & (y < end_ref[f])
        row_scale = jnp.broadcast_to(jnp.where(inside, row_taper, 0.0) * corr_row, (fh, TILE))
        turn = ca & (TILE - 1)
        base = jnp.clip(group * tiles - (ca >> 7), -tiles, tiles + 1) + tiles + 1
        spots.append((ra & 7, ra >> 3, turn, base, row_scale))
    for p in range(local):
        whole = turned.at[p, pl.ds(tiles + 1, tiles)]
        pltpu.make_async_copy(whole, whole, sent.at[small + p]).wait()

    def place(j):
        bands = strips * height // 8
        total = [None] * bands
        for p in range(local):
            lift, drop, turn, base, row_scale = spots[p]
            spread = [
                scale[jnp.clip(base + (i - tiles - 1), 0, tiles - 1)] for i in (j - 1, j)
            ]
            spread = pltpu.roll(
                jnp.where(lane[:8] >= TILE - turn, *(jnp.broadcast_to(w, (8, TILE)) for w in spread)), turn, axis=1
            )
            piece = jnp.where(lane >= TILE - turn, turned[p, base + (j - 1)], turned[p, base + j])
            piece = pltpu.roll(piece, turn, axis=1) * row_scale
            zero = jnp.zeros((8, TILE), jnp.float32)
            rows, held = [], zero
            for row in range(0, fh, 8):
                band = pltpu.roll(piece[row : row + 8] * spread, lift, axis=0)
                rows.append(jnp.where(sub < lift, held, band))
                held = band
            rows.append(jnp.where(sub < lift, held, 0.0))
            step = 1
            while step <= bands - fh // 8:
                rows = rows + [zero] * min(step, bands - len(rows))
                moved = [zero] * min(step, bands) + rows
                rows = [jnp.where((drop & step) != 0, new, old) for new, old in zip(moved, rows)]
                step *= 2
            total = [band if old is None else old + band for old, band in zip(total, rows)]
        for s in range(strips):
            for i in range(height // 8):
                blocks[s // lanes, s % lanes, j, pl.ds(i * 8, 8), :] = total[s * (height // 8) + i]

    def open_early():
        for t in range(levels - 1):
            d = dest(t)
            target, slot = route(t)

            @pl.when(jnp.logical_not(is_fed(t)))
            def _():
                f_copy(d, target, slot, blocks.at[d, :, pl.ds(0, early)]).start()

    def open_chunk(c):
        @pl.when(lax.rem(group, 2) == 0)
        def _():
            for k in range(1, lanes):
                x_copy(k, dest(0), c).start()

    openers = [lambda: open_chunk(0), open_early] + [
        functools.partial(open_chunk, c) for c in range(1, len(chunks))
    ]
    for i, (first, count) in enumerate([chunks[0], parts[0]] + chunks[1:]):
        for j in range(first, first + count):
            place(j)
            if j == first and i == 1:
                enter()
            if j == first and i > 0:
                openers[i - 1]()
    openers[-1]()

    @pl.when(lax.rem(group, 2) == 0)
    def _():
        for t in range(1, levels):
            for c in range(len(chunks)):
                for k in range(1, lanes):
                    x_copy(k, dest(t) if t < levels - 1 else z, c).start()

    hear(0, (z == 1) & high)
    hear(1, (z == levels - 2) & low)

    v = lax.broadcasted_iota(jnp.int32, (height, 1), 0) + strip * height
    u8 = lax.broadcasted_iota(jnp.int32, (8, fw), 1) + group * fw
    inv[...] = jnp.zeros_like(inv)

    def add_facet(f, carry):
        row_pos = v - row_ref[f]
        row_inside = (row_pos >= first_ref[f]) & (row_pos < end_ref[f])
        row_part = jnp.where(row_inside, taper(row_pos, fh), 0.0)
        col_pos = u8 - col_ref[f]
        col_inside = (col_pos >= 0) & (col_pos < fw)
        col_part = jnp.where(col_inside, taper(col_pos, fw), 0.0)
        for j in range(tiles):
            for row in range(0, height, 8):
                inv[j, pl.ds(row, 8), :] += (
                    row_part[row : row + 8] * col_part[:, j * TILE : (j + 1) * TILE]
                )
        return carry

    lax.fori_loop(0, facets, add_facet, 0)
    inv[...] = 1.0 / jnp.maximum(inv[...], 0.5)

    @pl.when(lax.rem(group, 2) == 1)
    def _():
        for t in range(0, levels):
            for c in range(len(chunks)):
                for k in range(1, lanes):
                    x_copy(k, dest(t) if t < levels - 1 else z, c).start()

    hear(0, (z > 1) & high)
    hear(1, (z < levels - 2) & low)

    def gather_x(d, c):
        total = blocks[d, x, span(c)]
        for k in range(1, lanes):
            x_copy(k, d, c).wait_recv()
            total = total + xrecv[k - 1, d, span(c)]
        return total

    def pass_early(t):
        d = dest(t)
        target, slot = route(t)

        @pl.when(is_fed(t))
        def _():
            f_copy(d, z, inlet(t)).wait_recv()
            fsend[d] = blocks[d, :, pl.ds(0, early)] + frecv[inlet(t)]
            f_copy(d, target, slot).start()

    def pass_rest(t):
        d = dest(t)
        target, slot = route(t)
        for c in range(len(chunks)):
            zsend[d, span(c)] = gather_x(d, c)

            @pl.when(is_fed(t))
            def _():
                z_copy(d, c, z, inlet(t)).wait_recv()
                zsend[d, span(c)] += zrecv[inlet(t), span(c)]

            z_copy(d, c, target, slot).start()

    def swap_early():
        fkeep[...] = blocks[z, :, pl.ds(0, early)]
        for level, there in sources():

            @pl.when(there)
            def _():
                f_copy(z, z, level).wait_recv()
                fkeep[...] += frecv[level]

        for k in range(1, lanes):
            fxsend[k - 1] = fkeep[lane_of(k)]
        for k in range(1, lanes):
            g_copy(k).start()

    def settle(i, total):
        first, count = parts[i]
        stitched = total * inv[pl.ds(first, count)]
        for j in range(count):
            out_ref[:, pl.ds((first + j) * TILE, TILE)] = stitched[j]
        psend[pl.ds(first, count)] = jnp.sum(stitched * stitched, axis=1, keepdims=True)
        for k in range(1, strips):
            p_copy(k, i).start()

    for t in range(levels - 1):
        pass_rest(t)
        if t == 0:
            for u in range(levels - 1):
                pass_early(u)
    swap_early()
    hear(0, (z > 0) & jnp.logical_not(high) & (levels > 1))
    hear(1, (z < levels - 1) & jnp.logical_not(low) & (levels > 1))

    for c in range(len(chunks)):
        zsend[z, span(c)] = blocks[z, x, span(c)]
        for level, there in sources():

            @pl.when(there)
            def _():
                z_copy(z, c, z, level).wait_recv()
                zsend[z, span(c)] += zrecv[level, span(c)]

        total = zsend[z, span(c)]
        for k in range(1, lanes):
            x_copy(k, z, c).wait_recv()
            total = total + xrecv[k - 1, z, span(c)]
        settle(1 + c, total)
    total = fkeep[x]
    for k in range(1, lanes):
        g_copy(k).wait_recv()
        total = total + fxrecv[k - 1]
    settle(0, total)

    def drain(i, ref):
        pltpu.make_async_remote_copy(
            src_ref=ref, dst_ref=ref, send_sem=sent.at[i], recv_sem=sent.at[i],
            device_id=at(z, x), device_id_type=MESH,
        ).wait_send()

    rest = pl.ds(early, tiles - early)
    if lanes > 1:
        drain(0, xrecv.at[:, :, rest])
        drain(3, fxsend)
    if levels > 1:
        drain(1, zsend.at[pl.ds(0, levels - 1), rest])
        drain(2, fsend.at[pl.ds(0, levels - 1)])
    if strips > 1:
        drain(4, precv)

    for i in list(range(1, len(parts))) + [0]:
        first, count = parts[i]
        if strips > 1:
            came = precv.at[:, pl.ds(first, count)]
            pltpu.make_async_remote_copy(
                src_ref=came, dst_ref=came, send_sem=sent.at[4], recv_sem=pr_sem.at[i],
                device_id=at(z, x), device_id_type=MESH,
            ).wait_recv()
        total = psend[pl.ds(first, count)]
        for k in range(1, strips):
            total = total + precv[k - 1, pl.ds(first, count)]
        total = total * (1.0 / (strips * height))
        for j in range(count):
            power_ref[pl.ds(first + j, 1), :] = total[j]


def finish(stitched_ref, power_ref, out_ref, power_out, sems):
    copies = [
        pltpu.make_async_copy(stitched_ref, out_ref, sems.at[0]),
        pltpu.make_async_copy(power_ref, power_out, sems.at[1]),
    ]
    for copy in copies:
        copy.start()
    for copy in copies:
        copy.wait()


def body(strips, lanes, residuals, corr_rows, corr_cols, row_anchor, col_anchor, first, end, slots):
    local, fh, fw = residuals.shape
    height = fh // 4
    levels = strips // lanes
    others = max(lanes - 1, 1)
    vmem = pl.BlockSpec(memory_space=pltpu.VMEM)
    hbm = pl.BlockSpec(memory_space=pltpu.HBM)
    dma = pltpu.SemaphoreType.DMA
    tiles = fw // TILE
    early = max(round(EARLY * tiles), 1)
    chunks = len(column_chunks(tiles, early))
    slots_in = max([len(table) for table in inlets(levels)] + [1])
    block_bytes = 4 * height * fw
    margin = 4 * 1024 * 1024
    blocks = 14 * local + (2 + others) * strips + 5 * levels + 4
    stitched, power = pl.pallas_call(
        functools.partial(kernel, strips, lanes),
        out_shape=(
            jax.ShapeDtypeStruct((height, fw), jnp.float32),
            jax.ShapeDtypeStruct((tiles, TILE), jnp.float32),
        ),
        in_specs=[hbm] * 8,
        out_specs=(vmem, vmem),
        scratch_shapes=[pltpu.SMEM(slots.shape, jnp.int32)] * 5
        + [
            pltpu.VMEM((1, fh), jnp.float32),
            pltpu.VMEM((tiles, TILE), jnp.float32),
            pltpu.VMEM((tiles, 1, TILE), jnp.float32),
            pltpu.VMEM((local, 3 * tiles + 2, fh, TILE), jnp.float32),
            pltpu.VMEM((levels, lanes, tiles, height, TILE), jnp.float32),
            pltpu.VMEM((tiles, height, TILE), jnp.float32),
            pltpu.VMEM((others, levels, tiles, height, TILE), jnp.float32),
            pltpu.VMEM((levels, tiles, height, TILE), jnp.float32),
            pltpu.VMEM((slots_in, tiles, height, TILE), jnp.float32),
            pltpu.VMEM((levels, lanes, early, height, TILE), jnp.float32),
            pltpu.VMEM((slots_in, lanes, early, height, TILE), jnp.float32),
            pltpu.VMEM((lanes, early, height, TILE), jnp.float32),
            pltpu.VMEM((others, early, height, TILE), jnp.float32),
            pltpu.VMEM((others, early, height, TILE), jnp.float32),
            pltpu.VMEM((tiles, 1, TILE), jnp.float32),
            pltpu.VMEM((strips - 1, tiles, 1, TILE), jnp.float32),
            pltpu.SemaphoreType.REGULAR((2,)),
            dma((7 + local,)),
            dma((others, levels, chunks)),
            dma((slots_in, chunks)),
            dma((slots_in,)),
            dma((others,)),
            dma((chunks + 1,)),
        ],
        compiler_params=pltpu.CompilerParams(
            collective_id=0,
            has_side_effects=True,
            vmem_limit_bytes=blocks * block_bytes + margin,
        ),
    )(*(
        pltpu.with_memory_space_constraint(operand, pltpu.HBM)
        for operand in (
            slots, row_anchor, col_anchor, first, end,
            corr_rows[None, :], corr_cols.reshape(fw // TILE, TILE), residuals,
        )
    ))
    stitched, power = pl.pallas_call(
        finish,
        out_shape=(
            jax.ShapeDtypeStruct((height, fw), jnp.float32),
            jax.ShapeDtypeStruct((fw // TILE, TILE), jnp.float32),
        ),
        in_specs=[vmem, vmem],
        out_specs=(hbm, hbm),
        scratch_shapes=[dma((2,))],
    )(*(pltpu.with_memory_space_constraint(part, pltpu.VMEM) for part in (stitched, power)))
    return stitched, power.reshape(fw)


def solution(mesh):
    strips = mesh.shape["strip"]
    lanes = math.gcd(strips, max(mesh.shape["col"] // 2, 1))
    in_specs = (P("strip", None, None), P(), P(), P(), P(), P(), P(), P())
    out_specs = (P("strip", "col"), P("col"))
    run = functools.partial(body, strips, lanes)
    return jax.shard_map(run, mesh=mesh, in_specs=in_specs, out_specs=out_specs, check_vma=False)
```

```python
import functools
import math

import jax
import jax.numpy as jnp
from jax import lax
from jax.experimental import pallas as pl
from jax.experimental.pallas import tpu as pltpu
from jax.sharding import PartitionSpec as P

MESH = pl.DeviceIdType.MESH
SHARES = (4, 5, 4, 4)
EARLY = 0.15
TILE = 128


def taper(position, count):
    angle = (position.astype(jnp.float32) + (0.5 - count / 2)) * (math.pi / count)
    square = angle * angle
    value = jnp.full_like(square, 1.0 / math.factorial(12))
    for order in (10, 8, 6, 4, 2, 0):
        sign = -1.0 if order % 4 == 2 else 1.0
        value = value * square + sign / math.factorial(order)
    return value * value


def fed(levels, z, d):
    return (z == 1 < d) or (z == levels - 2 > d)


def visit_order(levels):
    return [
        sorted((d for d in range(levels) if d != z), key=lambda d: (fed(levels, z, d), -abs(d - z)))
        for z in range(levels)
    ]


def inlets(levels):
    def inner(level):
        return 0 < level < levels - 1

    tables = []
    for z in range(levels):
        passed = [("pass", d) for d in range(levels) if d != z and fed(levels, z, d)]
        direct = [
            ("sum", s) for s in range(levels)
            if s != z and (inner(s) or (z == (1 if s == 0 else levels - 2)))
        ]
        tables.append(passed + direct)
    return tables


def column_chunks(tiles, first):
    ends = [sum(SHARES[:c]) for c in range(len(SHARES) + 1)]
    edges = [first + (tiles - first) * end // ends[-1] for end in ends]
    return [(a, b - a) for a, b in zip(edges, edges[1:]) if b > a]


def kernel(
    strips, lanes,
    slots_hbm, row_hbm, col_hbm, first_hbm, end_hbm, rows_hbm, cols_hbm, res_hbm,
    out_ref, power_ref,
    slots_ref, row_ref, col_ref, first_ref, end_ref, rows_ref, cols_ref, scale, turned, blocks, inv, xrecv, zsend, zrecv,
    fsend, frecv, fkeep, fxsend, fxrecv, psend, precv,
    line, sent, xr_sem, zr_sem, fr_sem, gr_sem, pr_sem,
):
    local, fh, fw = res_hbm.shape
    facets = slots_ref.shape[0]
    height = out_ref.shape[0]
    levels = strips // lanes
    tiles = fw // TILE
    early = fsend.shape[2]
    chunks = column_chunks(tiles, early)
    parts = [(0, early)] + chunks
    strip = lax.axis_index("strip")
    group = lax.axis_index("col")
    z, x = lax.div(strip, lanes), lax.rem(strip, lanes)

    low, high = z > 0, z < levels - 1
    leaf = jnp.logical_not(low & high)

    def at(level, lane):
        return {"strip": level * lanes + lane}

    barrier = pltpu.get_barrier_semaphore()
    for k in range(1, lanes):
        pl.semaphore_signal(barrier, device_id=at(z, lax.rem(x + k, lanes)), device_id_type=MESH)
    for there, step in ((low, -1), (high, 1)):

        @pl.when(there)
        def _():
            pl.semaphore_signal(barrier, device_id=at(z + step, x), device_id_type=MESH)

    sources = [
        (slots_hbm, slots_ref), (row_hbm, row_ref), (col_hbm, col_ref), (first_hbm, first_ref),
        (end_hbm, end_ref), (rows_hbm, rows_ref), (cols_hbm, cols_ref),
    ]
    small = len(sources)
    loads = [
        pltpu.make_async_copy(source, target, sent.at[i])
        for i, (source, target) in enumerate(sources)
    ]
    for load in loads:
        load.start()
    for p in range(local):
        for i in range(tiles):
            pltpu.make_async_copy(
                res_hbm.at[p, :, pl.ds(i * TILE, TILE)], turned.at[p, tiles + 1 + i], sent.at[small + p]
            ).start()

    def enter():
        pl.semaphore_wait(barrier, lanes - 1 + low.astype(jnp.int32) + high.astype(jnp.int32))
        for side, there, step in ((0, jnp.logical_not(low) & high, 1), (1, jnp.logical_not(high) & low, -1)):

            @pl.when(there)
            def _():
                pl.semaphore_signal(line.at[side], device_id=at(z + step, x), device_id_type=MESH)

    def hear(side, when):
        @pl.when(when)
        def _():
            pl.semaphore_wait(line.at[side], 1)

            @pl.when(high if side == 0 else low)
            def _():
                pl.semaphore_signal(
                    line.at[side], device_id=at(z + (1 if side == 0 else -1), x), device_id_type=MESH
                )

    order = visit_order(levels)

    def pick(values):
        value = jnp.int32(values[0])
        for level in range(1, levels):
            value = jnp.where(z == level, jnp.int32(values[level]), value)
        return value

    def dest(t):
        return pick([row[t] for row in order])

    def is_fed(t):
        return pick([int(fed(levels, level, row[t])) for level, row in enumerate(order)]) == 1

    tables = inlets(levels)
    leaves = {0: min(1, levels - 1), levels - 1: max(levels - 2, 0)}

    def route(t):
        targets, slots = [], []
        for level, row in enumerate(order):
            target = leaves.get(level, row[t])
            kind = ("sum", level) if target == row[t] else ("pass", row[t])
            targets.append(target)
            slots.append(tables[target].index(kind))
        return pick(targets), pick(slots)

    def inlet(t):
        return pick([
            tables[level].index(("pass", row[t])) if fed(levels, level, row[t]) else 0
            for level, row in enumerate(order)
        ])

    def sources():
        for i in range(max(len(table) for table in tables)):
            which = [i < len(table) and table[i][0] == "sum" for table in tables]
            if any(which):
                yield i, pick([int(there) for there in which]) == 1

    def lane_of(k):
        return lax.rem(x + k, lanes)

    def span(c):
        return pl.ds(chunks[c][0], chunks[c][1])

    def x_copy(k, d, c):
        return pltpu.make_async_remote_copy(
            src_ref=blocks.at[d, lane_of(k), span(c)],
            dst_ref=xrecv.at[k - 1, d, span(c)],
            send_sem=sent.at[0],
            recv_sem=xr_sem.at[k - 1, d, c],
            device_id=at(z, lane_of(k)),
            device_id_type=MESH,
        )

    def z_copy(d, c, target, slot):
        return pltpu.make_async_remote_copy(
            src_ref=zsend.at[d, span(c)],
            dst_ref=zrecv.at[slot, span(c)],
            send_sem=sent.at[1],
            recv_sem=zr_sem.at[slot, c],
            device_id=at(target, x),
            device_id_type=MESH,
        )

    def f_copy(d, target, slot, source=None):
        return pltpu.make_async_remote_copy(
            src_ref=fsend.at[d] if source is None else source,
            dst_ref=frecv.at[slot],
            send_sem=sent.at[2],
            recv_sem=fr_sem.at[slot],
            device_id=at(target, x),
            device_id_type=MESH,
        )

    def g_copy(k):
        return pltpu.make_async_remote_copy(
            src_ref=fxsend.at[k - 1],
            dst_ref=fxrecv.at[k - 1],
            send_sem=sent.at[3],
            recv_sem=gr_sem.at[k - 1],
            device_id=at(z, lane_of(k)),
            device_id_type=MESH,
        )

    def p_copy(k, i):
        return pltpu.make_async_remote_copy(
            src_ref=psend.at[pl.ds(*parts[i])],
            dst_ref=precv.at[k - 1, pl.ds(*parts[i])],
            send_sem=sent.at[4],
            recv_sem=pr_sem.at[i],
            device_id={"strip": lax.rem(strip + k, strips)},
            device_id_type=MESH,
        )

    eye = lax.broadcasted_iota(jnp.int32, (fh, fh), 0) == lax.broadcasted_iota(
        jnp.int32, (fh, fh), 1
    )
    y = lax.broadcasted_iota(jnp.int32, (fh, 1), 0)
    u = lax.broadcasted_iota(jnp.int32, (1, fw), 1)
    row_taper = taper(y, fh)
    col_taper = taper(u, fw)
    lane = lax.broadcasted_iota(jnp.int32, (fh, TILE), 1)
    sub = lax.broadcasted_iota(jnp.int32, (8, TILE), 0)
    blank = jnp.zeros((fh, TILE), jnp.float32)
    for p in range(local):
        for i in range(tiles + 1):
            turned[p, i] = blank
            turned[p, 2 * tiles + 1 + i] = blank
    for load in loads:
        load.wait()
    corr_row = jnp.sum(jnp.where(eye, rows_ref[...], 0.0), axis=1, keepdims=True)
    for i in range(tiles):
        columns = slice(i * TILE, (i + 1) * TILE)
        scale[i] = col_taper[:, columns] * cols_ref[pl.ds(i, 1), :]
    spots = []
    for p in range(local):
        f = slots_ref[strip * local + p]
        ra, ca = row_ref[f], col_ref[f]
        inside = (y >= first_ref[f]) & (y < end_ref[f])
        row_scale = jnp.broadcast_to(jnp.where(inside, row_taper, 0.0) * corr_row, (fh, TILE))
        turn = ca & (TILE - 1)
        base = jnp.clip(group * tiles - (ca >> 7), -tiles, tiles + 1) + tiles + 1
        spots.append((ra & 7, ra >> 3, turn, base, row_scale))
    for p in range(local):
        whole = turned.at[p, pl.ds(tiles + 1, tiles)]
        pltpu.make_async_copy(whole, whole, sent.at[small + p]).wait()

    def place(j):
        bands = strips * height // 8
        total = [None] * bands
        for p in range(local):
            lift, drop, turn, base, row_scale = spots[p]
            spread = [
                scale[jnp.clip(base + (i - tiles - 1), 0, tiles - 1)] for i in (j - 1, j)
            ]
            spread = pltpu.roll(
                jnp.where(lane[:8] >= TILE - turn, *(jnp.broadcast_to(w, (8, TILE)) for w in spread)), turn, axis=1
            )
            piece = jnp.where(lane >= TILE - turn, turned[p, base + (j - 1)], turned[p, base + j])
            piece = pltpu.roll(piece, turn, axis=1) * row_scale
            zero = jnp.zeros((8, TILE), jnp.float32)
            rows, held = [], zero
            for row in range(0, fh, 8):
                band = pltpu.roll(piece[row : row + 8] * spread, lift, axis=0)
                rows.append(jnp.where(sub < lift, held, band))
                held = band
            rows.append(jnp.where(sub < lift, held, 0.0))
            step = 1
            while step <= bands - fh // 8:
                rows = rows + [zero] * min(step, bands - len(rows))
                moved = [zero] * min(step, bands) + rows
                rows = [jnp.where((drop & step) != 0, new, old) for new, old in zip(moved, rows)]
                step *= 2
            total = [band if old is None else old + band for old, band in zip(total, rows)]
        for s in range(strips):
            for i in range(height // 8):
                blocks[s // lanes, s % lanes, j, pl.ds(i * 8, 8), :] = total[s * (height // 8) + i]

    def open_early():
        for t in range(levels - 1):
            d = dest(t)
            target, slot = route(t)

            @pl.when(jnp.logical_not(is_fed(t)))
            def _():
                f_copy(d, target, slot, blocks.at[d, :, pl.ds(0, early)]).start()

    def open_chunk(c):
        if c < 1:
            for k in range(1, lanes):
                x_copy(k, dest(0), c).start()
            return

        @pl.when(lax.rem(group, 2) == 0)
        def _():
            for k in range(1, lanes):
                x_copy(k, dest(0), c).start()

    openers = [lambda: open_chunk(0), open_early] + [
        functools.partial(open_chunk, c) for c in range(1, len(chunks))
    ]
    for i, (first, count) in enumerate([chunks[0], parts[0]] + chunks[1:]):
        for j in range(first, first + count):
            place(j)
            if j == first and i == 1:
                enter()
            if j == first and i > 0:
                openers[i - 1]()
    openers[-1]()

    @pl.when(lax.rem(group, 2) == 0)
    def _():
        for t in range(1, levels):
            for c in range(len(chunks)):
                for k in range(1, lanes):
                    x_copy(k, dest(t) if t < levels - 1 else z, c).start()

    hear(0, (z == 1) & high)
    hear(1, (z == levels - 2) & low)

    v = lax.broadcasted_iota(jnp.int32, (height, 1), 0) + strip * height
    u8 = lax.broadcasted_iota(jnp.int32, (8, fw), 1) + group * fw
    inv[...] = jnp.zeros_like(inv)

    def add_facet(f, carry):
        row_pos = v - row_ref[f]
        row_inside = (row_pos >= first_ref[f]) & (row_pos < end_ref[f])
        row_part = jnp.where(row_inside, taper(row_pos, fh), 0.0)
        col_pos = u8 - col_ref[f]
        col_inside = (col_pos >= 0) & (col_pos < fw)
        col_part = jnp.where(col_inside, taper(col_pos, fw), 0.0)
        for j in range(tiles):
            for row in range(0, height, 8):
                inv[j, pl.ds(row, 8), :] += (
                    row_part[row : row + 8] * col_part[:, j * TILE : (j + 1) * TILE]
                )
        return carry

    lax.fori_loop(0, facets, add_facet, 0)
    inv[...] = 1.0 / jnp.maximum(inv[...], 0.5)

    @pl.when(lax.rem(group, 2) == 1)
    def _():
        for t in range(0, levels):
            for c in range(1 if t == 0 else 0, len(chunks)):
                for k in range(1, lanes):
                    x_copy(k, dest(t) if t < levels - 1 else z, c).start()

    hear(0, (z > 1) & high)
    hear(1, (z < levels - 2) & low)

    def gather_x(d, c):
        total = blocks[d, x, span(c)]
        for k in range(1, lanes):
            x_copy(k, d, c).wait_recv()
            total = total + xrecv[k - 1, d, span(c)]
        return total

    def pass_early(t):
        d = dest(t)
        target, slot = route(t)

        @pl.when(is_fed(t))
        def _():
            f_copy(d, z, inlet(t)).wait_recv()
            fsend[d] = blocks[d, :, pl.ds(0, early)] + frecv[inlet(t)]
            f_copy(d, target, slot).start()

    def pass_rest(t):
        d = dest(t)
        target, slot = route(t)
        for c in range(len(chunks)):
            zsend[d, span(c)] = gather_x(d, c)

            @pl.when(is_fed(t))
            def _():
                z_copy(d, c, z, inlet(t)).wait_recv()
                zsend[d, span(c)] += zrecv[inlet(t), span(c)]

            z_copy(d, c, target, slot).start()

    def swap_early():
        fkeep[...] = blocks[z, :, pl.ds(0, early)]
        for level, there in sources():

            @pl.when(there)
            def _():
                f_copy(z, z, level).wait_recv()
                fkeep[...] += frecv[level]

        for k in range(1, lanes):
            fxsend[k - 1] = fkeep[lane_of(k)]
        for k in range(1, lanes):
            g_copy(k).start()

    def settle(i, total):
        first, count = parts[i]
        stitched = total * inv[pl.ds(first, count)]
        for j in range(count):
            out_ref[:, pl.ds((first + j) * TILE, TILE)] = stitched[j]
        psend[pl.ds(first, count)] = jnp.sum(stitched * stitched, axis=1, keepdims=True)
        for k in range(1, strips):
            p_copy(k, i).start()

    for t in range(levels - 1):
        pass_rest(t)
        if t == 0:
            for u in range(levels - 1):
                pass_early(u)
    swap_early()
    hear(0, (z > 0) & jnp.logical_not(high) & (levels > 1))
    hear(1, (z < levels - 1) & jnp.logical_not(low) & (levels > 1))

    for c in range(len(chunks)):
        zsend[z, span(c)] = blocks[z, x, span(c)]
        for level, there in sources():

            @pl.when(there)
            def _():
                z_copy(z, c, z, level).wait_recv()
                zsend[z, span(c)] += zrecv[level, span(c)]

        total = zsend[z, span(c)]
        for k in range(1, lanes):
            x_copy(k, z, c).wait_recv()
            total = total + xrecv[k - 1, z, span(c)]
        settle(1 + c, total)
    total = fkeep[x]
    for k in range(1, lanes):
        g_copy(k).wait_recv()
        total = total + fxrecv[k - 1]
    settle(0, total)

    def drain(i, ref):
        pltpu.make_async_remote_copy(
            src_ref=ref, dst_ref=ref, send_sem=sent.at[i], recv_sem=sent.at[i],
            device_id=at(z, x), device_id_type=MESH,
        ).wait_send()

    rest = pl.ds(early, tiles - early)
    if lanes > 1:
        drain(0, xrecv.at[:, :, rest])
        drain(3, fxsend)
    if levels > 1:
        drain(1, zsend.at[pl.ds(0, levels - 1), rest])
        drain(2, fsend.at[pl.ds(0, levels - 1)])
    if strips > 1:
        drain(4, precv)

    for i in list(range(1, len(parts))) + [0]:
        first, count = parts[i]
        if strips > 1:
            came = precv.at[:, pl.ds(first, count)]
            pltpu.make_async_remote_copy(
                src_ref=came, dst_ref=came, send_sem=sent.at[4], recv_sem=pr_sem.at[i],
                device_id=at(z, x), device_id_type=MESH,
            ).wait_recv()
        total = psend[pl.ds(first, count)]
        for k in range(1, strips):
            total = total + precv[k - 1, pl.ds(first, count)]
        total = total * (1.0 / (strips * height))
        for j in range(count):
            power_ref[pl.ds(first + j, 1), :] = total[j]


def finish(stitched_ref, power_ref, out_ref, power_out, sems):
    copies = [
        pltpu.make_async_copy(stitched_ref, out_ref, sems.at[0]),
        pltpu.make_async_copy(power_ref, power_out, sems.at[1]),
    ]
    for copy in copies:
        copy.start()
    for copy in copies:
        copy.wait()


def body(strips, lanes, residuals, corr_rows, corr_cols, row_anchor, col_anchor, first, end, slots):
    local, fh, fw = residuals.shape
    height = fh // 4
    levels = strips // lanes
    others = max(lanes - 1, 1)
    vmem = pl.BlockSpec(memory_space=pltpu.VMEM)
    hbm = pl.BlockSpec(memory_space=pltpu.HBM)
    dma = pltpu.SemaphoreType.DMA
    tiles = fw // TILE
    early = max(round(EARLY * tiles), 1)
    chunks = len(column_chunks(tiles, early))
    slots_in = max([len(table) for table in inlets(levels)] + [1])
    block_bytes = 4 * height * fw
    margin = 4 * 1024 * 1024
    blocks = 14 * local + (2 + others) * strips + 5 * levels + 4
    stitched, power = pl.pallas_call(
        functools.partial(kernel, strips, lanes),
        out_shape=(
            jax.ShapeDtypeStruct((height, fw), jnp.float32),
            jax.ShapeDtypeStruct((tiles, TILE), jnp.float32),
        ),
        in_specs=[hbm] * 8,
        out_specs=(vmem, vmem),
        scratch_shapes=[pltpu.SMEM(slots.shape, jnp.int32)] * 5
        + [
            pltpu.VMEM((1, fh), jnp.float32),
            pltpu.VMEM((tiles, TILE), jnp.float32),
            pltpu.VMEM((tiles, 1, TILE), jnp.float32),
            pltpu.VMEM((local, 3 * tiles + 2, fh, TILE), jnp.float32),
            pltpu.VMEM((levels, lanes, tiles, height, TILE), jnp.float32),
            pltpu.VMEM((tiles, height, TILE), jnp.float32),
            pltpu.VMEM((others, levels, tiles, height, TILE), jnp.float32),
            pltpu.VMEM((levels, tiles, height, TILE), jnp.float32),
            pltpu.VMEM((slots_in, tiles, height, TILE), jnp.float32),
            pltpu.VMEM((levels, lanes, early, height, TILE), jnp.float32),
            pltpu.VMEM((slots_in, lanes, early, height, TILE), jnp.float32),
            pltpu.VMEM((lanes, early, height, TILE), jnp.float32),
            pltpu.VMEM((others, early, height, TILE), jnp.float32),
            pltpu.VMEM((others, early, height, TILE), jnp.float32),
            pltpu.VMEM((tiles, 1, TILE), jnp.float32),
            pltpu.VMEM((strips - 1, tiles, 1, TILE), jnp.float32),
            pltpu.SemaphoreType.REGULAR((2,)),
            dma((7 + local,)),
            dma((others, levels, chunks)),
            dma((slots_in, chunks)),
            dma((slots_in,)),
            dma((others,)),
            dma((chunks + 1,)),
        ],
        compiler_params=pltpu.CompilerParams(
            collective_id=0,
            has_side_effects=True,
            vmem_limit_bytes=blocks * block_bytes + margin,
        ),
    )(*(
        pltpu.with_memory_space_constraint(operand, pltpu.HBM)
        for operand in (
            slots, row_anchor, col_anchor, first, end,
            corr_rows[None, :], corr_cols.reshape(fw // TILE, TILE), residuals,
        )
    ))
    stitched, power = pl.pallas_call(
        finish,
        out_shape=(
            jax.ShapeDtypeStruct((height, fw), jnp.float32),
            jax.ShapeDtypeStruct((fw // TILE, TILE), jnp.float32),
        ),
        in_specs=[vmem, vmem],
        out_specs=(hbm, hbm),
        scratch_shapes=[dma((2,))],
    )(*(pltpu.with_memory_space_constraint(part, pltpu.VMEM) for part in (stitched, power)))
    return stitched, power.reshape(fw)


def solution(mesh):
    strips = mesh.shape["strip"]
    lanes = math.gcd(strips, max(mesh.shape["col"] // 2, 1))
    in_specs = (P("strip", None, None), P(), P(), P(), P(), P(), P(), P())
    out_specs = (P("strip", "col"), P("col"))
    run = functools.partial(body, strips, lanes)
    return jax.shard_map(run, mesh=mesh, in_specs=in_specs, out_specs=out_specs, check_vma=False)
```

```python
import functools
import math

import jax
import jax.numpy as jnp
from jax import lax
from jax.experimental import pallas as pl
from jax.experimental.pallas import tpu as pltpu
from jax.sharding import PartitionSpec as P

MESH = pl.DeviceIdType.MESH
SHARES = (4, 5, 4, 4)
EARLY = 0.15
TILE = 128


def taper(position, count):
    angle = (position.astype(jnp.float32) + (0.5 - count / 2)) * (math.pi / count)
    square = angle * angle
    value = jnp.full_like(square, 1.0 / math.factorial(12))
    for order in (10, 8, 6, 4, 2, 0):
        sign = -1.0 if order % 4 == 2 else 1.0
        value = value * square + sign / math.factorial(order)
    return value * value


def fed(levels, z, d):
    return (z == 1 < d) or (z == levels - 2 > d)


def visit_order(levels):
    return [
        sorted((d for d in range(levels) if d != z), key=lambda d: (fed(levels, z, d), -abs(d - z)))
        for z in range(levels)
    ]


def inlets(levels):
    def inner(level):
        return 0 < level < levels - 1

    tables = []
    for z in range(levels):
        passed = [("pass", d) for d in range(levels) if d != z and fed(levels, z, d)]
        direct = [
            ("sum", s) for s in range(levels)
            if s != z and (inner(s) or (z == (1 if s == 0 else levels - 2)))
        ]
        tables.append(passed + direct)
    return tables


def column_chunks(tiles, first):
    ends = [sum(SHARES[:c]) for c in range(len(SHARES) + 1)]
    edges = [first + (tiles - first) * end // ends[-1] for end in ends]
    return [(a, b - a) for a, b in zip(edges, edges[1:]) if b > a]


def kernel(
    strips, lanes,
    slots_hbm, row_hbm, col_hbm, first_hbm, end_hbm, rows_hbm, cols_hbm, res_hbm,
    out_ref, power_ref,
    slots_ref, row_ref, col_ref, first_ref, end_ref, rows_ref, cols_ref, scale, turned, blocks, inv, xrecv, zsend, zrecv,
    fsend, frecv, fkeep, fxsend, fxrecv, psend, precv,
    line, sent, xr_sem, zr_sem, fr_sem, gr_sem, pr_sem,
):
    local, fh, fw = res_hbm.shape
    facets = slots_ref.shape[0]
    height = out_ref.shape[0]
    levels = strips // lanes
    tiles = fw // TILE
    early = fsend.shape[2]
    chunks = column_chunks(tiles, early)
    parts = [(0, early)] + chunks
    strip = lax.axis_index("strip")
    group = lax.axis_index("col")
    z, x = lax.div(strip, lanes), lax.rem(strip, lanes)

    low, high = z > 0, z < levels - 1
    leaf = jnp.logical_not(low & high)

    def at(level, lane):
        return {"strip": level * lanes + lane}

    barrier = pltpu.get_barrier_semaphore()
    for k in range(1, lanes):
        pl.semaphore_signal(barrier, device_id=at(z, lax.rem(x + k, lanes)), device_id_type=MESH)
    for there, step in ((low, -1), (high, 1)):

        @pl.when(there)
        def _():
            pl.semaphore_signal(barrier, device_id=at(z + step, x), device_id_type=MESH)

    sources = [
        (slots_hbm, slots_ref), (row_hbm, row_ref), (col_hbm, col_ref), (first_hbm, first_ref),
        (end_hbm, end_ref), (rows_hbm, rows_ref), (cols_hbm, cols_ref),
    ]
    small = len(sources)
    loads = [
        pltpu.make_async_copy(source, target, sent.at[i])
        for i, (source, target) in enumerate(sources)
    ]
    for load in loads:
        load.start()
    for p in range(local):
        for i in range(tiles):
            pltpu.make_async_copy(
                res_hbm.at[p, :, pl.ds(i * TILE, TILE)], turned.at[p, tiles + 1 + i], sent.at[small + p]
            ).start()

    def enter():
        pl.semaphore_wait(barrier, lanes - 1 + low.astype(jnp.int32) + high.astype(jnp.int32))
        for side, there, step in ((0, jnp.logical_not(low) & high, 1), (1, jnp.logical_not(high) & low, -1)):

            @pl.when(there)
            def _():
                pl.semaphore_signal(line.at[side], device_id=at(z + step, x), device_id_type=MESH)

    def hear(side, when):
        @pl.when(when)
        def _():
            pl.semaphore_wait(line.at[side], 1)

            @pl.when(high if side == 0 else low)
            def _():
                pl.semaphore_signal(
                    line.at[side], device_id=at(z + (1 if side == 0 else -1), x), device_id_type=MESH
                )

    order = visit_order(levels)

    def pick(values):
        value = jnp.int32(values[0])
        for level in range(1, levels):
            value = jnp.where(z == level, jnp.int32(values[level]), value)
        return value

    def dest(t):
        return pick([row[t] for row in order])

    def is_fed(t):
        return pick([int(fed(levels, level, row[t])) for level, row in enumerate(order)]) == 1

    tables = inlets(levels)
    leaves = {0: min(1, levels - 1), levels - 1: max(levels - 2, 0)}

    beyond = [
        [
            level not in leaves and not fed(levels, level, d) and abs(d - level) > 1 for d in row
        ]
        for level, row in enumerate(order)
    ]

    def is_beyond(t):
        return pick([int(row[t]) for row in beyond]) == 1

    def route(t):
        targets, slots = [], []
        for level, row in enumerate(order):
            target = leaves.get(level, row[t])
            kind = ("sum", level) if target == row[t] else ("pass", row[t])
            targets.append(target)
            slots.append(tables[target].index(kind))
        return pick(targets), pick(slots)

    def inlet(t):
        return pick([
            tables[level].index(("pass", row[t])) if fed(levels, level, row[t]) else 0
            for level, row in enumerate(order)
        ])

    def sources():
        for i in range(max(len(table) for table in tables)):
            which = [i < len(table) and table[i][0] == "sum" for table in tables]
            if any(which):
                yield i, pick([int(there) for there in which]) == 1

    def lane_of(k):
        return lax.rem(x + k, lanes)

    def span(c):
        return pl.ds(chunks[c][0], chunks[c][1])

    def x_copy(k, d, c):
        return pltpu.make_async_remote_copy(
            src_ref=blocks.at[d, lane_of(k), span(c)],
            dst_ref=xrecv.at[k - 1, d, span(c)],
            send_sem=sent.at[0],
            recv_sem=xr_sem.at[k - 1, d, c],
            device_id=at(z, lane_of(k)),
            device_id_type=MESH,
        )

    def z_copy(d, c, target, slot):
        return pltpu.make_async_remote_copy(
            src_ref=zsend.at[d, span(c)],
            dst_ref=zrecv.at[slot, span(c)],
            send_sem=sent.at[1],
            recv_sem=zr_sem.at[slot, c],
            device_id=at(target, x),
            device_id_type=MESH,
        )

    def f_copy(d, target, slot, source=None):
        return pltpu.make_async_remote_copy(
            src_ref=fsend.at[d] if source is None else source,
            dst_ref=frecv.at[slot],
            send_sem=sent.at[2],
            recv_sem=fr_sem.at[slot],
            device_id=at(target, x),
            device_id_type=MESH,
        )

    def g_copy(k):
        return pltpu.make_async_remote_copy(
            src_ref=fxsend.at[k - 1],
            dst_ref=fxrecv.at[k - 1],
            send_sem=sent.at[3],
            recv_sem=gr_sem.at[k - 1],
            device_id=at(z, lane_of(k)),
            device_id_type=MESH,
        )

    def p_copy(k, i):
        return pltpu.make_async_remote_copy(
            src_ref=psend.at[pl.ds(*parts[i])],
            dst_ref=precv.at[k - 1, pl.ds(*parts[i])],
            send_sem=sent.at[4],
            recv_sem=pr_sem.at[i],
            device_id={"strip": lax.rem(strip + k, strips)},
            device_id_type=MESH,
        )

    eye = lax.broadcasted_iota(jnp.int32, (fh, fh), 0) == lax.broadcasted_iota(
        jnp.int32, (fh, fh), 1
    )
    y = lax.broadcasted_iota(jnp.int32, (fh, 1), 0)
    u = lax.broadcasted_iota(jnp.int32, (1, fw), 1)
    row_taper = taper(y, fh)
    col_taper = taper(u, fw)
    lane = lax.broadcasted_iota(jnp.int32, (fh, TILE), 1)
    sub = lax.broadcasted_iota(jnp.int32, (8, TILE), 0)
    blank = jnp.zeros((fh, TILE), jnp.float32)
    for p in range(local):
        for i in range(tiles + 1):
            turned[p, i] = blank
            turned[p, 2 * tiles + 1 + i] = blank
    for load in loads:
        load.wait()
    corr_row = jnp.sum(jnp.where(eye, rows_ref[...], 0.0), axis=1, keepdims=True)
    for i in range(tiles):
        columns = slice(i * TILE, (i + 1) * TILE)
        scale[i] = col_taper[:, columns] * cols_ref[pl.ds(i, 1), :]
    spots = []
    for p in range(local):
        f = slots_ref[strip * local + p]
        ra, ca = row_ref[f], col_ref[f]
        inside = (y >= first_ref[f]) & (y < end_ref[f])
        row_scale = jnp.broadcast_to(jnp.where(inside, row_taper, 0.0) * corr_row, (fh, TILE))
        turn = ca & (TILE - 1)
        base = jnp.clip(group * tiles - (ca >> 7), -tiles, tiles + 1) + tiles + 1
        spots.append((ra & 7, ra >> 3, turn, base, row_scale))
    for p in range(local):
        whole = turned.at[p, pl.ds(tiles + 1, tiles)]
        pltpu.make_async_copy(whole, whole, sent.at[small + p]).wait()

    def place(j):
        bands = strips * height // 8
        total = [None] * bands
        for p in range(local):
            lift, drop, turn, base, row_scale = spots[p]
            spread = [
                scale[jnp.clip(base + (i - tiles - 1), 0, tiles - 1)] for i in (j - 1, j)
            ]
            spread = pltpu.roll(
                jnp.where(lane[:8] >= TILE - turn, *(jnp.broadcast_to(w, (8, TILE)) for w in spread)), turn, axis=1
            )
            piece = jnp.where(lane >= TILE - turn, turned[p, base + (j - 1)], turned[p, base + j])
            piece = pltpu.roll(piece, turn, axis=1) * row_scale
            zero = jnp.zeros((8, TILE), jnp.float32)
            rows, held = [], zero
            for row in range(0, fh, 8):
                band = pltpu.roll(piece[row : row + 8] * spread, lift, axis=0)
                rows.append(jnp.where(sub < lift, held, band))
                held = band
            rows.append(jnp.where(sub < lift, held, 0.0))
            step = 1
            while step <= bands - fh // 8:
                rows = rows + [zero] * min(step, bands - len(rows))
                moved = [zero] * min(step, bands) + rows
                rows = [jnp.where((drop & step) != 0, new, old) for new, old in zip(moved, rows)]
                step *= 2
            total = [band if old is None else old + band for old, band in zip(total, rows)]
        for s in range(strips):
            for i in range(height // 8):
                blocks[s // lanes, s % lanes, j, pl.ds(i * 8, 8), :] = total[s * (height // 8) + i]

    def open_early():
        for t in range(levels - 1):
            d = dest(t)
            target, slot = route(t)

            held = is_fed(t)
            if any(row[t] for row in beyond):
                held = held | is_beyond(t)

            @pl.when(jnp.logical_not(held))
            def _():
                f_copy(d, target, slot, blocks.at[d, :, pl.ds(0, early)]).start()

    def open_chunk(c):
        if c < 1:
            for k in range(1, lanes):
                x_copy(k, dest(0), c).start()
            return

        @pl.when(lax.rem(group, 2) == 0)
        def _():
            for k in range(1, lanes):
                x_copy(k, dest(0), c).start()

    openers = [lambda: open_chunk(0), open_early] + [
        functools.partial(open_chunk, c) for c in range(1, len(chunks))
    ]
    for i, (first, count) in enumerate([chunks[0], parts[0]] + chunks[1:]):
        for j in range(first, first + count):
            place(j)
            if j == first and i == 1:
                enter()
            if j == first and i > 0:
                openers[i - 1]()
    openers[-1]()

    @pl.when(lax.rem(group, 2) == 0)
    def _():
        for t in range(1, levels):
            for c in range(len(chunks)):
                for k in range(1, lanes):
                    x_copy(k, dest(t) if t < levels - 1 else z, c).start()

    hear(0, (z == 1) & high)
    hear(1, (z == levels - 2) & low)

    v = lax.broadcasted_iota(jnp.int32, (height, 1), 0) + strip * height
    u8 = lax.broadcasted_iota(jnp.int32, (8, fw), 1) + group * fw
    inv[...] = jnp.zeros_like(inv)

    def add_facet(f, carry):
        row_pos = v - row_ref[f]
        row_inside = (row_pos >= first_ref[f]) & (row_pos < end_ref[f])
        row_part = jnp.where(row_inside, taper(row_pos, fh), 0.0)
        col_pos = u8 - col_ref[f]
        col_inside = (col_pos >= 0) & (col_pos < fw)
        col_part = jnp.where(col_inside, taper(col_pos, fw), 0.0)
        for j in range(tiles):
            for row in range(0, height, 8):
                inv[j, pl.ds(row, 8), :] += (
                    row_part[row : row + 8] * col_part[:, j * TILE : (j + 1) * TILE]
                )
        return carry

    lax.fori_loop(0, facets, add_facet, 0)
    inv[...] = 1.0 / jnp.maximum(inv[...], 0.5)

    @pl.when(lax.rem(group, 2) == 1)
    def _():
        for t in range(0, levels):
            for c in range(1 if t == 0 else 0, len(chunks)):
                for k in range(1, lanes):
                    x_copy(k, dest(t) if t < levels - 1 else z, c).start()

    hear(0, (z > 1) & high)
    hear(1, (z < levels - 2) & low)

    def gather_x(d, c):
        total = blocks[d, x, span(c)]
        for k in range(1, lanes):
            x_copy(k, d, c).wait_recv()
            total = total + xrecv[k - 1, d, span(c)]
        return total

    def pass_early(t):
        d = dest(t)
        target, slot = route(t)

        @pl.when(is_fed(t))
        def _():
            f_copy(d, z, inlet(t)).wait_recv()
            fsend[d] = blocks[d, :, pl.ds(0, early)] + frecv[inlet(t)]
            f_copy(d, target, slot).start()

        if any(row[t] for row in beyond):

            @pl.when(is_beyond(t))
            def _():
                f_copy(d, target, slot, blocks.at[d, :, pl.ds(0, early)]).start()

    def pass_rest(t):
        d = dest(t)
        target, slot = route(t)
        for c in range(len(chunks)):
            zsend[d, span(c)] = gather_x(d, c)

            @pl.when(is_fed(t))
            def _():
                z_copy(d, c, z, inlet(t)).wait_recv()
                zsend[d, span(c)] += zrecv[inlet(t), span(c)]

            z_copy(d, c, target, slot).start()

    def swap_early():
        fkeep[...] = blocks[z, :, pl.ds(0, early)]
        for level, there in sources():

            @pl.when(there)
            def _():
                f_copy(z, z, level).wait_recv()
                fkeep[...] += frecv[level]

        for k in range(1, lanes):
            fxsend[k - 1] = fkeep[lane_of(k)]
        for k in range(1, lanes):
            g_copy(k).start()

    def settle(i, total):
        first, count = parts[i]
        stitched = total * inv[pl.ds(first, count)]
        for j in range(count):
            out_ref[:, pl.ds((first + j) * TILE, TILE)] = stitched[j]
        psend[pl.ds(first, count)] = jnp.sum(stitched * stitched, axis=1, keepdims=True)
        for k in range(1, strips):
            p_copy(k, i).start()

    for t in range(levels - 1):
        pass_rest(t)
        if t == 0:
            for u in range(levels - 1):
                pass_early(u)
    swap_early()
    hear(0, (z > 0) & jnp.logical_not(high) & (levels > 1))
    hear(1, (z < levels - 1) & jnp.logical_not(low) & (levels > 1))

    for c in range(len(chunks)):
        zsend[z, span(c)] = blocks[z, x, span(c)]
        for level, there in sources():

            @pl.when(there)
            def _():
                z_copy(z, c, z, level).wait_recv()
                zsend[z, span(c)] += zrecv[level, span(c)]

        total = zsend[z, span(c)]
        for k in range(1, lanes):
            x_copy(k, z, c).wait_recv()
            total = total + xrecv[k - 1, z, span(c)]
        settle(1 + c, total)
    total = fkeep[x]
    for k in range(1, lanes):
        g_copy(k).wait_recv()
        total = total + fxrecv[k - 1]
    settle(0, total)

    def drain(i, ref):
        pltpu.make_async_remote_copy(
            src_ref=ref, dst_ref=ref, send_sem=sent.at[i], recv_sem=sent.at[i],
            device_id=at(z, x), device_id_type=MESH,
        ).wait_send()

    rest = pl.ds(early, tiles - early)
    if lanes > 1:
        drain(0, xrecv.at[:, :, rest])
        drain(3, fxsend)
    if levels > 1:
        drain(1, zsend.at[pl.ds(0, levels - 1), rest])
        drain(2, fsend.at[pl.ds(0, levels - 1)])
    if strips > 1:
        drain(4, precv)

    for i in list(range(1, len(parts))) + [0]:
        first, count = parts[i]
        if strips > 1:
            came = precv.at[:, pl.ds(first, count)]
            pltpu.make_async_remote_copy(
                src_ref=came, dst_ref=came, send_sem=sent.at[4], recv_sem=pr_sem.at[i],
                device_id=at(z, x), device_id_type=MESH,
            ).wait_recv()
        total = psend[pl.ds(first, count)]
        for k in range(1, strips):
            total = total + precv[k - 1, pl.ds(first, count)]
        total = total * (1.0 / (strips * height))
        for j in range(count):
            power_ref[pl.ds(first + j, 1), :] = total[j]


def finish(stitched_ref, power_ref, out_ref, power_out, sems):
    copies = [
        pltpu.make_async_copy(stitched_ref, out_ref, sems.at[0]),
        pltpu.make_async_copy(power_ref, power_out, sems.at[1]),
    ]
    for copy in copies:
        copy.start()
    for copy in copies:
        copy.wait()


def body(strips, lanes, residuals, corr_rows, corr_cols, row_anchor, col_anchor, first, end, slots):
    local, fh, fw = residuals.shape
    height = fh // 4
    levels = strips // lanes
    others = max(lanes - 1, 1)
    vmem = pl.BlockSpec(memory_space=pltpu.VMEM)
    hbm = pl.BlockSpec(memory_space=pltpu.HBM)
    dma = pltpu.SemaphoreType.DMA
    tiles = fw // TILE
    early = max(round(EARLY * tiles), 1)
    chunks = len(column_chunks(tiles, early))
    slots_in = max([len(table) for table in inlets(levels)] + [1])
    block_bytes = 4 * height * fw
    margin = 4 * 1024 * 1024
    blocks = 14 * local + (2 + others) * strips + 5 * levels + 4
    stitched, power = pl.pallas_call(
        functools.partial(kernel, strips, lanes),
        out_shape=(
            jax.ShapeDtypeStruct((height, fw), jnp.float32),
            jax.ShapeDtypeStruct((tiles, TILE), jnp.float32),
        ),
        in_specs=[hbm] * 8,
        out_specs=(vmem, vmem),
        scratch_shapes=[pltpu.SMEM(slots.shape, jnp.int32)] * 5
        + [
            pltpu.VMEM((1, fh), jnp.float32),
            pltpu.VMEM((tiles, TILE), jnp.float32),
            pltpu.VMEM((tiles, 1, TILE), jnp.float32),
            pltpu.VMEM((local, 3 * tiles + 2, fh, TILE), jnp.float32),
            pltpu.VMEM((levels, lanes, tiles, height, TILE), jnp.float32),
            pltpu.VMEM((tiles, height, TILE), jnp.float32),
            pltpu.VMEM((others, levels, tiles, height, TILE), jnp.float32),
            pltpu.VMEM((levels, tiles, height, TILE), jnp.float32),
            pltpu.VMEM((slots_in, tiles, height, TILE), jnp.float32),
            pltpu.VMEM((levels, lanes, early, height, TILE), jnp.float32),
            pltpu.VMEM((slots_in, lanes, early, height, TILE), jnp.float32),
            pltpu.VMEM((lanes, early, height, TILE), jnp.float32),
            pltpu.VMEM((others, early, height, TILE), jnp.float32),
            pltpu.VMEM((others, early, height, TILE), jnp.float32),
            pltpu.VMEM((tiles, 1, TILE), jnp.float32),
            pltpu.VMEM((strips - 1, tiles, 1, TILE), jnp.float32),
            pltpu.SemaphoreType.REGULAR((2,)),
            dma((7 + local,)),
            dma((others, levels, chunks)),
            dma((slots_in, chunks)),
            dma((slots_in,)),
            dma((others,)),
            dma((chunks + 1,)),
        ],
        compiler_params=pltpu.CompilerParams(
            collective_id=0,
            has_side_effects=True,
            vmem_limit_bytes=blocks * block_bytes + margin,
        ),
    )(*(
        pltpu.with_memory_space_constraint(operand, pltpu.HBM)
        for operand in (
            slots, row_anchor, col_anchor, first, end,
            corr_rows[None, :], corr_cols.reshape(fw // TILE, TILE), residuals,
        )
    ))
    stitched, power = pl.pallas_call(
        finish,
        out_shape=(
            jax.ShapeDtypeStruct((height, fw), jnp.float32),
            jax.ShapeDtypeStruct((fw // TILE, TILE), jnp.float32),
        ),
        in_specs=[vmem, vmem],
        out_specs=(hbm, hbm),
        scratch_shapes=[dma((2,))],
    )(*(pltpu.with_memory_space_constraint(part, pltpu.VMEM) for part in (stitched, power)))
    return stitched, power.reshape(fw)


def solution(mesh):
    strips = mesh.shape["strip"]
    lanes = math.gcd(strips, max(mesh.shape["col"] // 2, 1))
    in_specs = (P("strip", None, None), P(), P(), P(), P(), P(), P(), P())
    out_specs = (P("strip", "col"), P("col"))
    run = functools.partial(body, strips, lanes)
    return jax.shard_map(run, mesh=mesh, in_specs=in_specs, out_specs=out_specs, check_vma=False)
```

```python
import functools
import math

import jax
import jax.numpy as jnp
from jax import lax
from jax.experimental import pallas as pl
from jax.experimental.pallas import tpu as pltpu
from jax.sharding import PartitionSpec as P

MESH = pl.DeviceIdType.MESH
SHARES = (4, 5, 4, 4)
EARLY = 0.15
TILE = 128


def taper(position, count):
    angle = (position.astype(jnp.float32) + (0.5 - count / 2)) * (math.pi / count)
    square = angle * angle
    value = jnp.full_like(square, 1.0 / math.factorial(12))
    for order in (10, 8, 6, 4, 2, 0):
        sign = -1.0 if order % 4 == 2 else 1.0
        value = value * square + sign / math.factorial(order)
    return value * value


def fed(levels, z, d):
    return (z == 1 < d) or (z == levels - 2 > d)


def visit_order(levels):
    return [
        sorted((d for d in range(levels) if d != z), key=lambda d: (fed(levels, z, d), -abs(d - z)))
        for z in range(levels)
    ]


def inlets(levels):
    def inner(level):
        return 0 < level < levels - 1

    tables = []
    for z in range(levels):
        passed = [("pass", d) for d in range(levels) if d != z and fed(levels, z, d)]
        direct = [
            ("sum", s) for s in range(levels)
            if s != z and (inner(s) or (z == (1 if s == 0 else levels - 2)))
        ]
        tables.append(passed + direct)
    return tables


def column_chunks(tiles, first):
    ends = [sum(SHARES[:c]) for c in range(len(SHARES) + 1)]
    edges = [first + (tiles - first) * end // ends[-1] for end in ends]
    return [(a, b - a) for a, b in zip(edges, edges[1:]) if b > a]


def kernel(strips, lanes, *refs):
    pl.run_scoped(
        functools.partial(exchange, strips, lanes, *refs), pltpu.SemaphoreType.DMA((7 + refs[7].shape[0],))
    )


def exchange(
    strips, lanes,
    slots_hbm, row_hbm, col_hbm, first_hbm, end_hbm, rows_hbm, cols_hbm, res_hbm,
    out_ref, power_ref,
    slots_ref, row_ref, col_ref, first_ref, end_ref, rows_ref, cols_ref, scale, turned, blocks, inv, xrecv, zsend, zrecv,
    fsend, frecv, fkeep, fxsend, fxrecv, psend, precv,
    line, xr_sem, zr_sem, fr_sem, gr_sem, pr_sem, sent,
):
    local, fh, fw = res_hbm.shape
    facets = slots_ref.shape[0]
    height = out_ref.shape[0]
    levels = strips // lanes
    tiles = fw // TILE
    early = fsend.shape[2]
    chunks = column_chunks(tiles, early)
    parts = [(0, early)] + chunks
    last = len(parts) - 1
    batch_of = [1 if i == 0 else 2 if i == last else 0 for i in range(len(parts))]
    batches = [(0, early, chunks[-1][0] - early), (2, *chunks[-1]), (1, *parts[0])][last < 2 :]
    strip = lax.axis_index("strip")
    group = lax.axis_index("col")
    z, x = lax.div(strip, lanes), lax.rem(strip, lanes)

    low, high = z > 0, z < levels - 1
    leaf = jnp.logical_not(low & high)

    def at(level, lane):
        return {"strip": level * lanes + lane}

    barrier = pltpu.get_barrier_semaphore()
    for k in range(1, lanes):
        pl.semaphore_signal(barrier, device_id=at(z, lax.rem(x + k, lanes)), device_id_type=MESH)
    for there, step in ((low, -1), (high, 1)):

        @pl.when(there)
        def _():
            pl.semaphore_signal(barrier, device_id=at(z + step, x), device_id_type=MESH)

    sources = [
        (slots_hbm, slots_ref), (row_hbm, row_ref), (col_hbm, col_ref), (first_hbm, first_ref),
        (end_hbm, end_ref), (rows_hbm, rows_ref), (cols_hbm, cols_ref),
    ]
    small = len(sources)
    loads = [
        pltpu.make_async_copy(source, target, sent.at[i])
        for i, (source, target) in enumerate(sources)
    ]
    for load in loads:
        load.start()
    for p in range(local):
        for i in range(tiles):
            pltpu.make_async_copy(
                res_hbm.at[p, :, pl.ds(i * TILE, TILE)], turned.at[p, tiles + 1 + i], sent.at[small + p]
            ).start()

    def enter():
        pl.semaphore_wait(barrier, lanes - 1 + low.astype(jnp.int32) + high.astype(jnp.int32))
        for side, there, step in ((0, jnp.logical_not(low) & high, 1), (1, jnp.logical_not(high) & low, -1)):

            @pl.when(there)
            def _():
                pl.semaphore_signal(line.at[side], device_id=at(z + step, x), device_id_type=MESH)

    def hear(side, when):
        @pl.when(when)
        def _():
            pl.semaphore_wait(line.at[side], 1)

            @pl.when(high if side == 0 else low)
            def _():
                pl.semaphore_signal(
                    line.at[side], device_id=at(z + (1 if side == 0 else -1), x), device_id_type=MESH
                )

    order = visit_order(levels)

    def pick(values):
        value = jnp.int32(values[0])
        for level in range(1, levels):
            value = jnp.where(z == level, jnp.int32(values[level]), value)
        return value

    def dest(t):
        return pick([row[t] for row in order])

    def is_fed(t):
        return pick([int(fed(levels, level, row[t])) for level, row in enumerate(order)]) == 1

    tables = inlets(levels)
    leaves = {0: min(1, levels - 1), levels - 1: max(levels - 2, 0)}

    beyond = [
        [
            level not in leaves and not fed(levels, level, d) and abs(d - level) > 1 for d in row
        ]
        for level, row in enumerate(order)
    ]

    def is_beyond(t):
        return pick([int(row[t]) for row in beyond]) == 1

    def route(t):
        targets, slots = [], []
        for level, row in enumerate(order):
            target = leaves.get(level, row[t])
            kind = ("sum", level) if target == row[t] else ("pass", row[t])
            targets.append(target)
            slots.append(tables[target].index(kind))
        return pick(targets), pick(slots)

    def inlet(t):
        return pick([
            tables[level].index(("pass", row[t])) if fed(levels, level, row[t]) else 0
            for level, row in enumerate(order)
        ])

    def sources():
        for i in range(max(len(table) for table in tables)):
            which = [i < len(table) and table[i][0] == "sum" for table in tables]
            if any(which):
                yield i, pick([int(there) for there in which]) == 1

    def lane_of(k):
        return lax.rem(x + k, lanes)

    def span(c):
        return pl.ds(chunks[c][0], chunks[c][1])

    def x_copy(k, d, c):
        return pltpu.make_async_remote_copy(
            src_ref=blocks.at[d, lane_of(k), span(c)],
            dst_ref=xrecv.at[k - 1, d, span(c)],
            send_sem=sent.at[0],
            recv_sem=xr_sem.at[k - 1, d, c],
            device_id=at(z, lane_of(k)),
            device_id_type=MESH,
        )

    def z_copy(d, c, target, slot):
        return pltpu.make_async_remote_copy(
            src_ref=zsend.at[d, span(c)],
            dst_ref=zrecv.at[slot, span(c)],
            send_sem=sent.at[1],
            recv_sem=zr_sem.at[slot, c],
            device_id=at(target, x),
            device_id_type=MESH,
        )

    def f_copy(d, target, slot, source=None):
        return pltpu.make_async_remote_copy(
            src_ref=fsend.at[d] if source is None else source,
            dst_ref=frecv.at[slot],
            send_sem=sent.at[2],
            recv_sem=fr_sem.at[slot],
            device_id=at(target, x),
            device_id_type=MESH,
        )

    def g_copy(k):
        return pltpu.make_async_remote_copy(
            src_ref=fxsend.at[k - 1],
            dst_ref=fxrecv.at[k - 1],
            send_sem=sent.at[3],
            recv_sem=gr_sem.at[k - 1],
            device_id=at(z, lane_of(k)),
            device_id_type=MESH,
        )

    def p_copy(k, i):
        return pltpu.make_async_remote_copy(
            src_ref=psend.at[pl.ds(*parts[i])],
            dst_ref=precv.at[k - 1, pl.ds(*parts[i])],
            send_sem=sent.at[4],
            recv_sem=pr_sem.at[batch_of[i]],
            device_id={"strip": lax.rem(strip + k, strips)},
            device_id_type=MESH,
        )

    eye = lax.broadcasted_iota(jnp.int32, (fh, fh), 0) == lax.broadcasted_iota(
        jnp.int32, (fh, fh), 1
    )
    y = lax.broadcasted_iota(jnp.int32, (fh, 1), 0)
    u = lax.broadcasted_iota(jnp.int32, (1, fw), 1)
    row_taper = taper(y, fh)
    col_taper = taper(u, fw)
    lane = lax.broadcasted_iota(jnp.int32, (fh, TILE), 1)
    sub = lax.broadcasted_iota(jnp.int32, (8, TILE), 0)
    blank = jnp.zeros((fh, TILE), jnp.float32)
    for p in range(local):
        for i in range(tiles + 1):
            turned[p, i] = blank
            turned[p, 2 * tiles + 1 + i] = blank
    for load in loads:
        load.wait()
    corr_row = jnp.sum(jnp.where(eye, rows_ref[...], 0.0), axis=1, keepdims=True)
    for i in range(tiles):
        columns = slice(i * TILE, (i + 1) * TILE)
        scale[i] = col_taper[:, columns] * cols_ref[pl.ds(i, 1), :]
    spots = []
    for p in range(local):
        f = slots_ref[strip * local + p]
        ra, ca = row_ref[f], col_ref[f]
        inside = (y >= first_ref[f]) & (y < end_ref[f])
        row_scale = jnp.broadcast_to(jnp.where(inside, row_taper, 0.0) * corr_row, (fh, TILE))
        turn = ca & (TILE - 1)
        base = jnp.clip(group * tiles - (ca >> 7), -tiles, tiles + 1) + tiles + 1
        spots.append((ra & 7, ra >> 3, turn, base, row_scale))
    for p in range(local):
        whole = turned.at[p, pl.ds(tiles + 1, tiles)]
        pltpu.make_async_copy(whole, whole, sent.at[small + p]).wait()

    def place(j):
        bands = strips * height // 8
        total = [None] * bands
        for p in range(local):
            lift, drop, turn, base, row_scale = spots[p]
            spread = [
                scale[jnp.clip(base + (i - tiles - 1), 0, tiles - 1)] for i in (j - 1, j)
            ]
            spread = pltpu.roll(
                jnp.where(lane[:8] >= TILE - turn, *(jnp.broadcast_to(w, (8, TILE)) for w in spread)), turn, axis=1
            )
            piece = jnp.where(lane >= TILE - turn, turned[p, base + (j - 1)], turned[p, base + j])
            piece = pltpu.roll(piece, turn, axis=1) * row_scale
            zero = jnp.zeros((8, TILE), jnp.float32)
            rows, held = [], zero
            for row in range(0, fh, 8):
                band = pltpu.roll(piece[row : row + 8] * spread, lift, axis=0)
                rows.append(jnp.where(sub < lift, held, band))
                held = band
            rows.append(jnp.where(sub < lift, held, 0.0))
            step = 1
            while step <= bands - fh // 8:
                rows = rows + [zero] * min(step, bands - len(rows))
                moved = [zero] * min(step, bands) + rows
                rows = [jnp.where((drop & step) != 0, new, old) for new, old in zip(moved, rows)]
                step *= 2
            total = [band if old is None else old + band for old, band in zip(total, rows)]
        for s in range(strips):
            for i in range(height // 8):
                blocks[s // lanes, s % lanes, j, pl.ds(i * 8, 8), :] = total[s * (height // 8) + i]

    def open_early():
        for t in range(levels - 1):
            d = dest(t)
            target, slot = route(t)

            held = is_fed(t)
            if any(row[t] for row in beyond):
                held = held | is_beyond(t)

            @pl.when(jnp.logical_not(held))
            def _():
                f_copy(d, target, slot, blocks.at[d, :, pl.ds(0, early)]).start()

    def open_chunk(c):
        if c < 1:
            for k in range(1, lanes):
                x_copy(k, dest(0), c).start()
            return

        @pl.when(lax.rem(group, 2) == 0)
        def _():
            for k in range(1, lanes):
                x_copy(k, dest(0), c).start()

    openers = [lambda: open_chunk(0), open_early] + [
        functools.partial(open_chunk, c) for c in range(1, len(chunks))
    ]
    for i, (first, count) in enumerate([chunks[0], parts[0]] + chunks[1:]):
        for j in range(first, first + count):
            place(j)
            if j == first and i == 1:
                enter()
            if j == first and i > 0:
                openers[i - 1]()
    openers[-1]()

    @pl.when(lax.rem(group, 2) == 0)
    def _():
        for t in range(1, levels):
            for c in range(len(chunks)):
                for k in range(1, lanes):
                    x_copy(k, dest(t) if t < levels - 1 else z, c).start()

    hear(0, (z == 1) & high)
    hear(1, (z == levels - 2) & low)

    v = lax.broadcasted_iota(jnp.int32, (height, 1), 0) + strip * height
    u8 = lax.broadcasted_iota(jnp.int32, (8, fw), 1) + group * fw
    inv[...] = jnp.zeros_like(inv)

    def add_facet(f, carry):
        row_pos = v - row_ref[f]
        row_inside = (row_pos >= first_ref[f]) & (row_pos < end_ref[f])
        row_part = jnp.where(row_inside, taper(row_pos, fh), 0.0)
        col_pos = u8 - col_ref[f]
        col_inside = (col_pos >= 0) & (col_pos < fw)
        col_part = jnp.where(col_inside, taper(col_pos, fw), 0.0)
        for j in range(tiles):
            for row in range(0, height, 8):
                inv[j, pl.ds(row, 8), :] += (
                    row_part[row : row + 8] * col_part[:, j * TILE : (j + 1) * TILE]
                )
        return carry

    lax.fori_loop(0, facets, add_facet, 0)
    inv[...] = 1.0 / jnp.maximum(inv[...], 0.5)

    @pl.when(lax.rem(group, 2) == 1)
    def _():
        for t in range(0, levels):
            for c in range(1 if t == 0 else 0, len(chunks)):
                for k in range(1, lanes):
                    x_copy(k, dest(t) if t < levels - 1 else z, c).start()

    hear(0, (z > 1) & high)
    hear(1, (z < levels - 2) & low)

    def gather_x(d, c):
        total = blocks[d, x, span(c)]
        for k in range(1, lanes):
            x_copy(k, d, c).wait_recv()
            total = total + xrecv[k - 1, d, span(c)]
        return total

    def pass_early(t):
        d = dest(t)
        target, slot = route(t)

        @pl.when(is_fed(t))
        def _():
            f_copy(d, z, inlet(t)).wait_recv()
            fsend[d] = blocks[d, :, pl.ds(0, early)] + frecv[inlet(t)]
            f_copy(d, target, slot).start()

        if any(row[t] for row in beyond):

            @pl.when(is_beyond(t))
            def _():
                f_copy(d, target, slot, blocks.at[d, :, pl.ds(0, early)]).start()

    def pass_rest(t):
        d = dest(t)
        target, slot = route(t)
        for c in range(len(chunks)):
            zsend[d, span(c)] = gather_x(d, c)

            @pl.when(is_fed(t))
            def _():
                z_copy(d, c, z, inlet(t)).wait_recv()
                zsend[d, span(c)] += zrecv[inlet(t), span(c)]

            z_copy(d, c, target, slot).start()

    def swap_early():
        fkeep[...] = blocks[z, :, pl.ds(0, early)]
        for level, there in sources():

            @pl.when(there)
            def _():
                f_copy(z, z, level).wait_recv()
                fkeep[...] += frecv[level]

        for k in range(1, lanes):
            fxsend[k - 1] = fkeep[lane_of(k)]
        for k in range(1, lanes):
            g_copy(k).start()

    def settle(i, total):
        first, count = parts[i]
        stitched = total * inv[pl.ds(first, count)]
        for j in range(count):
            out_ref[:, pl.ds((first + j) * TILE, TILE)] = stitched[j]
        psend[pl.ds(first, count)] = jnp.sum(stitched * stitched, axis=1, keepdims=True)
        for k in sorted(range(1, strips), key=lambda k: -min(k // lanes, levels - k // lanes)):
            p_copy(k, i).start()

    for t in range(levels - 1):
        pass_rest(t)
        if t == 0:
            for u in range(levels - 1):
                pass_early(u)
    swap_early()
    hear(0, (z > 0) & jnp.logical_not(high) & (levels > 1))
    hear(1, (z < levels - 1) & jnp.logical_not(low) & (levels > 1))

    for c in range(len(chunks)):
        zsend[z, span(c)] = blocks[z, x, span(c)]
        for level, there in sources():

            @pl.when(there)
            def _():
                z_copy(z, c, z, level).wait_recv()
                zsend[z, span(c)] += zrecv[level, span(c)]

        total = zsend[z, span(c)]
        for k in range(1, lanes):
            x_copy(k, z, c).wait_recv()
            total = total + xrecv[k - 1, z, span(c)]
        settle(1 + c, total)
    total = fkeep[x]
    for k in range(1, lanes):
        g_copy(k).wait_recv()
        total = total + fxrecv[k - 1]
    settle(0, total)

    def drain(i, ref):
        pltpu.make_async_remote_copy(
            src_ref=ref, dst_ref=ref, send_sem=sent.at[i], recv_sem=sent.at[i],
            device_id=at(z, x), device_id_type=MESH,
        ).wait_send()

    rest = pl.ds(early, tiles - early)
    if lanes > 1:
        drain(0, xrecv.at[:, :, rest])
        drain(3, fxsend)
    if levels > 1:
        drain(1, zsend.at[pl.ds(0, levels - 1), rest])
        drain(2, fsend.at[pl.ds(0, levels - 1)])
    if strips > 1:
        drain(4, precv)

    for i, first, count in batches:
        if strips > 1:
            came = precv.at[:, pl.ds(first, count)]
            pltpu.make_async_remote_copy(
                src_ref=came, dst_ref=came, send_sem=sent.at[4], recv_sem=pr_sem.at[i],
                device_id=at(z, x), device_id_type=MESH,
            ).wait_recv()
        total = psend[pl.ds(first, count)]
        for k in range(1, strips):
            total = total + precv[k - 1, pl.ds(first, count)]
        total = total * (1.0 / (strips * height))
        for j in range(count):
            power_ref[pl.ds(first + j, 1), :] = total[j]


def finish(stitched_ref, power_ref, out_ref, power_out, sems):
    copies = [
        pltpu.make_async_copy(stitched_ref, out_ref, sems.at[0]),
        pltpu.make_async_copy(power_ref, power_out, sems.at[1]),
    ]
    for copy in copies:
        copy.start()
    for copy in copies:
        copy.wait()


def body(strips, lanes, residuals, corr_rows, corr_cols, row_anchor, col_anchor, first, end, slots):
    local, fh, fw = residuals.shape
    height = fh // 4
    levels = strips // lanes
    others = max(lanes - 1, 1)
    vmem = pl.BlockSpec(memory_space=pltpu.VMEM)
    hbm = pl.BlockSpec(memory_space=pltpu.HBM)
    dma = pltpu.SemaphoreType.DMA
    tiles = fw // TILE
    early = max(round(EARLY * tiles), 1)
    chunks = len(column_chunks(tiles, early))
    slots_in = max([len(table) for table in inlets(levels)] + [1])
    block_bytes = 4 * height * fw
    margin = 4 * 1024 * 1024
    blocks = 14 * local + (2 + others) * strips + 5 * levels + 4
    stitched, power = pl.pallas_call(
        functools.partial(kernel, strips, lanes),
        out_shape=(
            jax.ShapeDtypeStruct((height, fw), jnp.float32),
            jax.ShapeDtypeStruct((tiles, TILE), jnp.float32),
        ),
        in_specs=[hbm] * 8,
        out_specs=(vmem, vmem),
        scratch_shapes=[pltpu.SMEM(slots.shape, jnp.int32)] * 5
        + [
            pltpu.VMEM((1, fh), jnp.float32),
            pltpu.VMEM((tiles, TILE), jnp.float32),
            pltpu.VMEM((tiles, 1, TILE), jnp.float32),
            pltpu.VMEM((local, 3 * tiles + 2, fh, TILE), jnp.float32),
            pltpu.VMEM((levels, lanes, tiles, height, TILE), jnp.float32),
            pltpu.VMEM((tiles, height, TILE), jnp.float32),
            pltpu.VMEM((others, levels, tiles, height, TILE), jnp.float32),
            pltpu.VMEM((levels, tiles, height, TILE), jnp.float32),
            pltpu.VMEM((slots_in, tiles, height, TILE), jnp.float32),
            pltpu.VMEM((levels, lanes, early, height, TILE), jnp.float32),
            pltpu.VMEM((slots_in, lanes, early, height, TILE), jnp.float32),
            pltpu.VMEM((lanes, early, height, TILE), jnp.float32),
            pltpu.VMEM((others, early, height, TILE), jnp.float32),
            pltpu.VMEM((others, early, height, TILE), jnp.float32),
            pltpu.VMEM((tiles, 1, TILE), jnp.float32),
            pltpu.VMEM((strips - 1, tiles, 1, TILE), jnp.float32),
            pltpu.SemaphoreType.REGULAR((2,)),
            dma((others, levels, chunks)),
            dma((slots_in, chunks)),
            dma((slots_in,)),
            dma((others,)),
            dma((3,)),
        ],
        compiler_params=pltpu.CompilerParams(
            collective_id=0,
            has_side_effects=True,
            vmem_limit_bytes=blocks * block_bytes + margin,
        ),
    )(*(
        pltpu.with_memory_space_constraint(operand, pltpu.HBM)
        for operand in (
            slots, row_anchor, col_anchor, first, end,
            corr_rows[None, :], corr_cols.reshape(fw // TILE, TILE), residuals,
        )
    ))
    stitched, power = pl.pallas_call(
        finish,
        out_shape=(
            jax.ShapeDtypeStruct((height, fw), jnp.float32),
            jax.ShapeDtypeStruct((fw // TILE, TILE), jnp.float32),
        ),
        in_specs=[vmem, vmem],
        out_specs=(hbm, hbm),
        scratch_shapes=[dma((2,))],
    )(*(pltpu.with_memory_space_constraint(part, pltpu.VMEM) for part in (stitched, power)))
    return stitched, power.reshape(fw)


def solution(mesh):
    strips = mesh.shape["strip"]
    lanes = math.gcd(strips, max(mesh.shape["col"] // 2, 1))
    in_specs = (P("strip", None, None), P(), P(), P(), P(), P(), P(), P())
    out_specs = (P("strip", "col"), P("col"))
    run = functools.partial(body, strips, lanes)
    return jax.shard_map(run, mesh=mesh, in_specs=in_specs, out_specs=out_specs, check_vma=False)
```

```python
import functools
import math

import jax
import jax.numpy as jnp
from jax import lax
from jax.experimental import pallas as pl
from jax.experimental.pallas import tpu as pltpu
from jax.sharding import PartitionSpec as P

MESH = pl.DeviceIdType.MESH
SHARES = (4, 5, 4, 4)
EARLY = 0.15
TILE = 128


def taper(position, count):
    angle = (position.astype(jnp.float32) + (0.5 - count / 2)) * (math.pi / count)
    square = angle * angle
    value = jnp.full_like(square, 1.0 / math.factorial(12))
    for order in (10, 8, 6, 4, 2, 0):
        sign = -1.0 if order % 4 == 2 else 1.0
        value = value * square + sign / math.factorial(order)
    return value * value


def fed(levels, z, d):
    return (z == 1 < d) or (z == levels - 2 > d)


def visit_order(levels):
    return [
        sorted((d for d in range(levels) if d != z), key=lambda d: (fed(levels, z, d), -abs(d - z)))
        for z in range(levels)
    ]


def inlets(levels):
    def inner(level):
        return 0 < level < levels - 1

    tables = []
    for z in range(levels):
        passed = [("pass", d) for d in range(levels) if d != z and fed(levels, z, d)]
        direct = [
            ("sum", s) for s in range(levels)
            if s != z and (inner(s) or (z == (1 if s == 0 else levels - 2)))
        ]
        tables.append(passed + direct)
    return tables


def column_chunks(tiles, first):
    ends = [sum(SHARES[:c]) for c in range(len(SHARES) + 1)]
    edges = [first + (tiles - first) * end // ends[-1] for end in ends]
    return [(a, b - a) for a, b in zip(edges, edges[1:]) if b > a]


def kernel(strips, lanes, *refs):
    pl.run_scoped(
        functools.partial(exchange, strips, lanes, *refs), pltpu.SemaphoreType.DMA((7 + refs[7].shape[0],))
    )


def exchange(
    strips, lanes,
    slots_hbm, row_hbm, col_hbm, first_hbm, end_hbm, rows_hbm, cols_hbm, res_hbm,
    out_ref, power_ref,
    slots_ref, row_ref, col_ref, first_ref, end_ref, rows_ref, cols_ref, scale, turned, blocks, inv, xrecv, zsend, zrecv,
    fsend, frecv, fkeep, fxsend, fxrecv, psend, precv,
    line, xr_sem, zr_sem, fr_sem, gr_sem, pr_sem, sent,
):
    local, fh, fw = res_hbm.shape
    facets = slots_ref.shape[0]
    height = out_ref.shape[0]
    levels = strips // lanes
    tiles = fw // TILE
    early = fsend.shape[2]
    chunks = column_chunks(tiles, early)
    parts = [(0, early)] + chunks
    last = len(parts) - 1
    batch_of = [1 if i == 0 else 2 if i == last else 0 for i in range(len(parts))]
    batches = [(0, early, chunks[-1][0] - early), (2, *chunks[-1]), (1, *parts[0])][last < 2 :]
    strip = lax.axis_index("strip")
    group = lax.axis_index("col")
    z, x = lax.div(strip, lanes), lax.rem(strip, lanes)

    low, high = z > 0, z < levels - 1
    leaf = jnp.logical_not(low & high)

    def at(level, lane):
        return {"strip": level * lanes + lane}

    barrier = pltpu.get_barrier_semaphore()
    for k in range(1, lanes):
        pl.semaphore_signal(barrier, device_id=at(z, lax.rem(x + k, lanes)), device_id_type=MESH)
    for there, step in ((low, -1), (high, 1)):

        @pl.when(there)
        def _():
            pl.semaphore_signal(barrier, device_id=at(z + step, x), device_id_type=MESH)

    sources = [
        (slots_hbm, slots_ref), (row_hbm, row_ref), (col_hbm, col_ref), (first_hbm, first_ref),
        (end_hbm, end_ref), (rows_hbm, rows_ref), (cols_hbm, cols_ref),
    ]
    small = len(sources)
    loads = [
        pltpu.make_async_copy(source, target, sent.at[i])
        for i, (source, target) in enumerate(sources)
    ]
    for p in range(local):
        for i in range(tiles):
            pltpu.make_async_copy(
                res_hbm.at[p, :, pl.ds(i * TILE, TILE)], turned.at[p, tiles + 1 + i], sent.at[small + p]
            ).start()
    for load in loads:
        load.start()

    def enter():
        pl.semaphore_wait(barrier, lanes - 1 + low.astype(jnp.int32) + high.astype(jnp.int32))
        for side, there, step in ((0, jnp.logical_not(low) & high, 1), (1, jnp.logical_not(high) & low, -1)):

            @pl.when(there)
            def _():
                pl.semaphore_signal(line.at[side], device_id=at(z + step, x), device_id_type=MESH)

    def hear(side, when):
        @pl.when(when)
        def _():
            pl.semaphore_wait(line.at[side], 1)

            @pl.when(high if side == 0 else low)
            def _():
                pl.semaphore_signal(
                    line.at[side], device_id=at(z + (1 if side == 0 else -1), x), device_id_type=MESH
                )

    order = visit_order(levels)

    def pick(values):
        value = jnp.int32(values[0])
        for level in range(1, levels):
            value = jnp.where(z == level, jnp.int32(values[level]), value)
        return value

    def dest(t):
        return pick([row[t] for row in order])

    def is_fed(t):
        return pick([int(fed(levels, level, row[t])) for level, row in enumerate(order)]) == 1

    tables = inlets(levels)
    leaves = {0: min(1, levels - 1), levels - 1: max(levels - 2, 0)}

    beyond = [
        [
            level not in leaves and not fed(levels, level, d) and abs(d - level) > 1 for d in row
        ]
        for level, row in enumerate(order)
    ]

    def is_beyond(t):
        return pick([int(row[t]) for row in beyond]) == 1

    def route(t):
        targets, slots = [], []
        for level, row in enumerate(order):
            target = leaves.get(level, row[t])
            kind = ("sum", level) if target == row[t] else ("pass", row[t])
            targets.append(target)
            slots.append(tables[target].index(kind))
        return pick(targets), pick(slots)

    def inlet(t):
        return pick([
            tables[level].index(("pass", row[t])) if fed(levels, level, row[t]) else 0
            for level, row in enumerate(order)
        ])

    def sources():
        for i in range(max(len(table) for table in tables)):
            which = [i < len(table) and table[i][0] == "sum" for table in tables]
            if any(which):
                yield i, pick([int(there) for there in which]) == 1

    def lane_of(k):
        return lax.rem(x + k, lanes)

    def span(c):
        return pl.ds(chunks[c][0], chunks[c][1])

    def x_copy(k, d, c):
        return pltpu.make_async_remote_copy(
            src_ref=blocks.at[d, lane_of(k), span(c)],
            dst_ref=xrecv.at[k - 1, d, span(c)],
            send_sem=sent.at[0],
            recv_sem=xr_sem.at[k - 1, d, c],
            device_id=at(z, lane_of(k)),
            device_id_type=MESH,
        )

    def z_copy(d, c, target, slot):
        return pltpu.make_async_remote_copy(
            src_ref=zsend.at[d, span(c)],
            dst_ref=zrecv.at[slot, span(c)],
            send_sem=sent.at[1],
            recv_sem=zr_sem.at[slot, c],
            device_id=at(target, x),
            device_id_type=MESH,
        )

    def f_copy(d, target, slot, source=None):
        return pltpu.make_async_remote_copy(
            src_ref=fsend.at[d] if source is None else source,
            dst_ref=frecv.at[slot],
            send_sem=sent.at[2],
            recv_sem=fr_sem.at[slot],
            device_id=at(target, x),
            device_id_type=MESH,
        )

    def g_copy(k):
        return pltpu.make_async_remote_copy(
            src_ref=fxsend.at[k - 1],
            dst_ref=fxrecv.at[k - 1],
            send_sem=sent.at[3],
            recv_sem=gr_sem.at[k - 1],
            device_id=at(z, lane_of(k)),
            device_id_type=MESH,
        )

    def p_copy(k, i):
        return pltpu.make_async_remote_copy(
            src_ref=psend.at[pl.ds(*parts[i])],
            dst_ref=precv.at[k - 1, pl.ds(*parts[i])],
            send_sem=sent.at[4],
            recv_sem=pr_sem.at[batch_of[i]],
            device_id={"strip": lax.rem(strip + k, strips)},
            device_id_type=MESH,
        )

    eye = lax.broadcasted_iota(jnp.int32, (fh, fh), 0) == lax.broadcasted_iota(
        jnp.int32, (fh, fh), 1
    )
    y = lax.broadcasted_iota(jnp.int32, (fh, 1), 0)
    u = lax.broadcasted_iota(jnp.int32, (1, fw), 1)
    row_taper = taper(y, fh)
    col_taper = taper(u, fw)
    lane = lax.broadcasted_iota(jnp.int32, (fh, TILE), 1)
    sub = lax.broadcasted_iota(jnp.int32, (8, TILE), 0)
    blank = jnp.zeros((fh, TILE), jnp.float32)
    for p in range(local):
        for i in range(tiles + 1):
            turned[p, i] = blank
            turned[p, 2 * tiles + 1 + i] = blank
    for load in loads:
        load.wait()
    corr_row = jnp.sum(jnp.where(eye, rows_ref[...], 0.0), axis=1, keepdims=True)
    for i in range(tiles):
        columns = slice(i * TILE, (i + 1) * TILE)
        scale[i] = col_taper[:, columns] * cols_ref[pl.ds(i, 1), :]
    spots = []
    for p in range(local):
        f = slots_ref[strip * local + p]
        ra, ca = row_ref[f], col_ref[f]
        inside = (y >= first_ref[f]) & (y < end_ref[f])
        row_scale = jnp.broadcast_to(jnp.where(inside, row_taper, 0.0) * corr_row, (fh, TILE))
        turn = ca & (TILE - 1)
        base = jnp.clip(group * tiles - (ca >> 7), -tiles, tiles + 1) + tiles + 1
        spots.append((ra & 7, ra >> 3, turn, base, row_scale))
    for p in range(local):
        whole = turned.at[p, pl.ds(tiles + 1, tiles)]
        pltpu.make_async_copy(whole, whole, sent.at[small + p]).wait()

    def place(j):
        bands = strips * height // 8
        total = [None] * bands
        for p in range(local):
            lift, drop, turn, base, row_scale = spots[p]
            spread = [
                scale[jnp.clip(base + (i - tiles - 1), 0, tiles - 1)] for i in (j - 1, j)
            ]
            spread = pltpu.roll(
                jnp.where(lane[:8] >= TILE - turn, *(jnp.broadcast_to(w, (8, TILE)) for w in spread)), turn, axis=1
            )
            piece = jnp.where(lane >= TILE - turn, turned[p, base + (j - 1)], turned[p, base + j])
            piece = pltpu.roll(piece, turn, axis=1) * row_scale
            zero = jnp.zeros((8, TILE), jnp.float32)
            rows, held = [], zero
            for row in range(0, fh, 8):
                band = pltpu.roll(piece[row : row + 8] * spread, lift, axis=0)
                rows.append(jnp.where(sub < lift, held, band))
                held = band
            rows.append(jnp.where(sub < lift, held, 0.0))
            step = 1
            while step <= bands - fh // 8:
                rows = rows + [zero] * min(step, bands - len(rows))
                moved = [zero] * min(step, bands) + rows
                rows = [jnp.where((drop & step) != 0, new, old) for new, old in zip(moved, rows)]
                step *= 2
            total = [band if old is None else old + band for old, band in zip(total, rows)]
        for s in range(strips):
            for i in range(height // 8):
                blocks[s // lanes, s % lanes, j, pl.ds(i * 8, 8), :] = total[s * (height // 8) + i]

    def open_early():
        for t in range(levels - 1):
            d = dest(t)
            target, slot = route(t)

            held = is_fed(t)
            if any(row[t] for row in beyond):
                held = held | is_beyond(t)

            @pl.when(jnp.logical_not(held))
            def _():
                f_copy(d, target, slot, blocks.at[d, :, pl.ds(0, early)]).start()

    def open_chunk(c):
        if c < 1:
            for k in range(1, lanes):
                x_copy(k, dest(0), c).start()
            return

        @pl.when(lax.rem(group, 2) == 0)
        def _():
            for k in range(1, lanes):
                x_copy(k, dest(0), c).start()

    openers = [lambda: open_chunk(0), open_early] + [
        functools.partial(open_chunk, c) for c in range(1, len(chunks))
    ]
    for i, (first, count) in enumerate([chunks[0], parts[0]] + chunks[1:]):
        for j in range(first, first + count):
            place(j)
            if j == first and i == 1:
                enter()
            if j == first and i > 0:
                openers[i - 1]()
    openers[-1]()

    @pl.when(lax.rem(group, 2) == 0)
    def _():
        for t in range(1, levels):
            for c in range(len(chunks)):
                for k in range(1, lanes):
                    x_copy(k, dest(t) if t < levels - 1 else z, c).start()

    hear(0, (z == 1) & high)
    hear(1, (z == levels - 2) & low)

    v = lax.broadcasted_iota(jnp.int32, (height, 1), 0) + strip * height
    u8 = lax.broadcasted_iota(jnp.int32, (8, fw), 1) + group * fw
    inv[...] = jnp.zeros_like(inv)

    def add_facet(f, carry):
        row_pos = v - row_ref[f]
        row_inside = (row_pos >= first_ref[f]) & (row_pos < end_ref[f])
        row_part = jnp.where(row_inside, taper(row_pos, fh), 0.0)
        col_pos = u8 - col_ref[f]
        col_inside = (col_pos >= 0) & (col_pos < fw)
        col_part = jnp.where(col_inside, taper(col_pos, fw), 0.0)
        for j in range(tiles):
            for row in range(0, height, 8):
                inv[j, pl.ds(row, 8), :] += (
                    row_part[row : row + 8] * col_part[:, j * TILE : (j + 1) * TILE]
                )
        return carry

    lax.fori_loop(0, facets, add_facet, 0)
    inv[...] = 1.0 / jnp.maximum(inv[...], 0.5)

    @pl.when(lax.rem(group, 2) == 1)
    def _():
        for t in range(0, levels):
            for c in range(1 if t == 0 else 0, len(chunks)):
                for k in range(1, lanes):
                    x_copy(k, dest(t) if t < levels - 1 else z, c).start()

    hear(0, (z > 1) & high)
    hear(1, (z < levels - 2) & low)

    def gather_x(d, c):
        total = blocks[d, x, span(c)]
        for k in range(1, lanes):
            x_copy(k, d, c).wait_recv()
            total = total + xrecv[k - 1, d, span(c)]
        return total

    def pass_early(t):
        d = dest(t)
        target, slot = route(t)

        @pl.when(is_fed(t))
        def _():
            f_copy(d, z, inlet(t)).wait_recv()
            fsend[d] = blocks[d, :, pl.ds(0, early)] + frecv[inlet(t)]
            f_copy(d, target, slot).start()

        if any(row[t] for row in beyond):

            @pl.when(is_beyond(t))
            def _():
                f_copy(d, target, slot, blocks.at[d, :, pl.ds(0, early)]).start()

    def pass_rest(t):
        d = dest(t)
        target, slot = route(t)
        for c in range(len(chunks)):
            zsend[d, span(c)] = gather_x(d, c)

            @pl.when(is_fed(t))
            def _():
                z_copy(d, c, z, inlet(t)).wait_recv()
                zsend[d, span(c)] += zrecv[inlet(t), span(c)]

            z_copy(d, c, target, slot).start()

    def swap_early():
        fkeep[...] = blocks[z, :, pl.ds(0, early)]
        for level, there in sources():

            @pl.when(there)
            def _():
                f_copy(z, z, level).wait_recv()
                fkeep[...] += frecv[level]

        for k in range(1, lanes):
            fxsend[k - 1] = fkeep[lane_of(k)]
        for k in range(1, lanes):
            g_copy(k).start()

    def settle(i, total):
        first, count = parts[i]
        stitched = total * inv[pl.ds(first, count)]
        for j in range(count):
            out_ref[:, pl.ds((first + j) * TILE, TILE)] = stitched[j]
        psend[pl.ds(first, count)] = jnp.sum(stitched * stitched, axis=1, keepdims=True)
        for k in sorted(range(1, strips), key=lambda k: -min(k // lanes, levels - k // lanes)):
            p_copy(k, i).start()

    for t in range(levels - 1):
        pass_rest(t)
        if t == 0:
            for u in range(levels - 1):
                pass_early(u)
    swap_early()
    hear(0, (z > 0) & jnp.logical_not(high) & (levels > 1))
    hear(1, (z < levels - 1) & jnp.logical_not(low) & (levels > 1))

    for c in range(len(chunks)):
        zsend[z, span(c)] = blocks[z, x, span(c)]
        for level, there in sources():

            @pl.when(there)
            def _():
                z_copy(z, c, z, level).wait_recv()
                zsend[z, span(c)] += zrecv[level, span(c)]

        total = zsend[z, span(c)]
        for k in range(1, lanes):
            x_copy(k, z, c).wait_recv()
            total = total + xrecv[k - 1, z, span(c)]
        settle(1 + c, total)
    total = fkeep[x]
    for k in range(1, lanes):
        g_copy(k).wait_recv()
        total = total + fxrecv[k - 1]
    settle(0, total)

    def drain(i, ref):
        pltpu.make_async_remote_copy(
            src_ref=ref, dst_ref=ref, send_sem=sent.at[i], recv_sem=sent.at[i],
            device_id=at(z, x), device_id_type=MESH,
        ).wait_send()

    rest = pl.ds(early, tiles - early)
    if lanes > 1:
        drain(0, xrecv.at[:, :, rest])
        drain(3, fxsend)
    if levels > 1:
        drain(1, zsend.at[pl.ds(0, levels - 1), rest])
        drain(2, fsend.at[pl.ds(0, levels - 1)])
    if strips > 1:
        drain(4, precv)

    for i, first, count in batches:
        if strips > 1:
            came = precv.at[:, pl.ds(first, count)]
            pltpu.make_async_remote_copy(
                src_ref=came, dst_ref=came, send_sem=sent.at[4], recv_sem=pr_sem.at[i],
                device_id=at(z, x), device_id_type=MESH,
            ).wait_recv()
        total = psend[pl.ds(first, count)]
        for k in range(1, strips):
            total = total + precv[k - 1, pl.ds(first, count)]
        total = total * (1.0 / (strips * height))
        for j in range(count):
            power_ref[pl.ds(first + j, 1), :] = total[j]


def finish(stitched_ref, power_ref, out_ref, power_out, sems):
    copies = [
        pltpu.make_async_copy(stitched_ref, out_ref, sems.at[0]),
        pltpu.make_async_copy(power_ref, power_out, sems.at[1]),
    ]
    for copy in copies:
        copy.start()
    for copy in copies:
        copy.wait()


def body(strips, lanes, residuals, corr_rows, corr_cols, row_anchor, col_anchor, first, end, slots):
    local, fh, fw = residuals.shape
    height = fh // 4
    levels = strips // lanes
    others = max(lanes - 1, 1)
    vmem = pl.BlockSpec(memory_space=pltpu.VMEM)
    hbm = pl.BlockSpec(memory_space=pltpu.HBM)
    dma = pltpu.SemaphoreType.DMA
    tiles = fw // TILE
    early = max(round(EARLY * tiles), 1)
    chunks = len(column_chunks(tiles, early))
    slots_in = max([len(table) for table in inlets(levels)] + [1])
    block_bytes = 4 * height * fw
    margin = 4 * 1024 * 1024
    blocks = 14 * local + (2 + others) * strips + 5 * levels + 4
    stitched, power = pl.pallas_call(
        functools.partial(kernel, strips, lanes),
        out_shape=(
            jax.ShapeDtypeStruct((height, fw), jnp.float32),
            jax.ShapeDtypeStruct((tiles, TILE), jnp.float32),
        ),
        in_specs=[hbm] * 8,
        out_specs=(vmem, vmem),
        scratch_shapes=[pltpu.SMEM(slots.shape, jnp.int32)] * 5
        + [
            pltpu.VMEM((1, fh), jnp.float32),
            pltpu.VMEM((tiles, TILE), jnp.float32),
            pltpu.VMEM((tiles, 1, TILE), jnp.float32),
            pltpu.VMEM((local, 3 * tiles + 2, fh, TILE), jnp.float32),
            pltpu.VMEM((levels, lanes, tiles, height, TILE), jnp.float32),
            pltpu.VMEM((tiles, height, TILE), jnp.float32),
            pltpu.VMEM((others, levels, tiles, height, TILE), jnp.float32),
            pltpu.VMEM((levels, tiles, height, TILE), jnp.float32),
            pltpu.VMEM((slots_in, tiles, height, TILE), jnp.float32),
            pltpu.VMEM((levels, lanes, early, height, TILE), jnp.float32),
            pltpu.VMEM((slots_in, lanes, early, height, TILE), jnp.float32),
            pltpu.VMEM((lanes, early, height, TILE), jnp.float32),
            pltpu.VMEM((others, early, height, TILE), jnp.float32),
            pltpu.VMEM((others, early, height, TILE), jnp.float32),
            pltpu.VMEM((tiles, 1, TILE), jnp.float32),
            pltpu.VMEM((strips - 1, tiles, 1, TILE), jnp.float32),
            pltpu.SemaphoreType.REGULAR((2,)),
            dma((others, levels, chunks)),
            dma((slots_in, chunks)),
            dma((slots_in,)),
            dma((others,)),
            dma((3,)),
        ],
        compiler_params=pltpu.CompilerParams(
            collective_id=0,
            has_side_effects=True,
            vmem_limit_bytes=blocks * block_bytes + margin,
        ),
    )(*(
        pltpu.with_memory_space_constraint(operand, pltpu.HBM)
        for operand in (
            slots, row_anchor, col_anchor, first, end,
            corr_rows[None, :], corr_cols.reshape(fw // TILE, TILE), residuals,
        )
    ))
    stitched, power = pl.pallas_call(
        finish,
        out_shape=(
            jax.ShapeDtypeStruct((height, fw), jnp.float32),
            jax.ShapeDtypeStruct((fw // TILE, TILE), jnp.float32),
        ),
        in_specs=[vmem, vmem],
        out_specs=(hbm, hbm),
        scratch_shapes=[dma((2,))],
    )(*(pltpu.with_memory_space_constraint(part, pltpu.VMEM) for part in (stitched, power)))
    return stitched, power.reshape(fw)


def solution(mesh):
    strips = mesh.shape["strip"]
    lanes = math.gcd(strips, max(mesh.shape["col"] // 2, 1))
    in_specs = (P("strip", None, None), P(), P(), P(), P(), P(), P(), P())
    out_specs = (P("strip", "col"), P("col"))
    run = functools.partial(body, strips, lanes)
    return jax.shard_map(run, mesh=mesh, in_specs=in_specs, out_specs=out_specs, check_vma=False)
```
